128 devices in a mesh: pb: 8 (over z, core), ka: 16 (over x, y).
Axes of the slice: x: 4, y: 4, z: 4, core: 2. Of those that a mesh axis runs over, the one named last changes fastest.
Arguments:
- queries: float32 [1, 16384, 128], P(None, ('pb', 'ka')), may hold values from -6 to 6
- keys: float32 [1, 16384, 128], P(None, ('ka', 'pb')), may hold values from -6 to 6
- values: float32 [1, 16384, 128], P(None, ('ka', 'pb')), may hold values from -6 to 6
- tangent_q: float32 [1, 16384, 128], P(None, ('pb', 'ka')), may hold values from -6 to 6
- tangent_k: float32 [1, 16384, 128], P(None, ('ka', 'pb')), may hold values from -6 to 6
- tangent_v: float32 [1, 16384, 128], P(None, ('ka', 'pb')), may hold values from -6 to 6
Outputs:
- attended: float32 [1, 16384, 128], P(None, ('pb', 'ka'))
- attended_tangent: float32 [1, 16384, 128], P(None, ('pb', 'ka'))
The draws below stay inside these ranges and needn't reach their ends.
All inputs are finite; a program needn't handle non-finite values.
Results may differ from the reference program's by a relative error of at most 0.0003.
Values sent between devices are 32-bit elements; how exact they have to be, the bound alone decides.
A program may use at most 128 MiB of HBM per device.

```python
import jax
import jax.numpy as jnp
from jax import lax

DH = 128
HEADS = 1
SEQ = 16384


def draw_queries(key, part):
    fresh = jax.random.fold_in(key, 1)
    return jnp.clip(jax.random.normal(fresh, (HEADS, SEQ, DH), jnp.float32), -6.0, 6.0)


def draw_keys(key, part):
    fresh = jax.random.fold_in(key, 2)
    return jnp.clip(jax.random.normal(fresh, (HEADS, SEQ, DH), jnp.float32), -6.0, 6.0)


def block_scale(own_key, shape, shards, least, largest):
    level, own = 1.0, jax.random.fold_in(own_key, 6)
    for axis_at, shards_of in shards:
        heights = jnp.exp(jax.random.uniform(jax.random.fold_in(own, axis_at), (shards_of,), jnp.float32, least / len(shards), largest / len(shards)))
        level = level * jnp.repeat(heights, shape[axis_at] // shards_of).reshape([-1 if axis == axis_at else 1 for axis in range(len(shape))])
    return level


def gaussian(rng, shape, spread, limit, shards=(), held_as=jnp.bfloat16):
    drawn = jax.random.normal(rng, shape, jnp.float32) * spread
    if len(shards) > 0:
        drawn = block_scale(rng, shape, shards, -0.22, 0.18) * drawn
    return jnp.clip(drawn, min=-limit, max=limit).astype(held_as)


def setup_inputs(seed: int = 0) -> dict:
    seeds = jax.random.split(jax.random.key(seed), 7)
    queries = draw_queries(jax.random.fold_in(seeds[6], 71), 0)
    keys = draw_keys(jax.random.fold_in(seeds[6], 71), 0)
    values = gaussian(seeds[2], (HEADS, SEQ, DH), 1.0, 6.0, ((1, 128),), jnp.float32)
    tangent_q = gaussian(seeds[3], (HEADS, SEQ, DH), 1.0, 6.0, ((1, 128),), jnp.float32)
    tangent_k = gaussian(seeds[4], (HEADS, SEQ, DH), 1.0, 6.0, ((1, 128),), jnp.float32)
    tangent_v = gaussian(seeds[5], (HEADS, SEQ, DH), 1.0, 6.0, ((1, 128),), jnp.float32)
    return dict(queries=queries, keys=keys, values=values, tangent_q=tangent_q, tangent_k=tangent_k, tangent_v=tangent_v)


def attend_block(query_blk, dquery_blk, head_keys, head_dkeys, head_values, head_dvalues):
    highest = lax.Precision.HIGHEST
    factor = DH ** -0.5
    scores = jnp.dot(query_blk, head_keys.T, precision=highest) * factor
    tangent = (jnp.dot(dquery_blk, head_keys.T, precision=highest) + jnp.dot(query_blk, head_dkeys.T, precision=highest)) * factor
    peak = jnp.max(scores, axis=1, keepdims=True)
    weights = jnp.exp(scores - peak)
    total = jnp.sum(weights, axis=1, keepdims=True)
    product = weights * tangent
    drift = jnp.sum(product, axis=1, keepdims=True) / total
    output = jnp.dot(weights, head_values, precision=highest) / total
    moved = (jnp.dot(weights, head_dvalues, precision=highest) + jnp.dot(product, head_values, precision=highest)) / total
    return output, moved - output * drift


def reference(queries, keys, values, tangent_q, tangent_k, tangent_v):
    block = min(1024, SEQ)
    count = SEQ // block

    def per_head(items):
        head_q, head_dq, head_k, head_dk, head_v, head_dv = items
        split_q = head_q.reshape(count, block, DH)
        split_dq = head_dq.reshape(count, block, DH)

        def per_block(pair):
            return attend_block(pair[0], pair[1], head_k, head_dk, head_v, head_dv)

        result = lax.map(per_block, (split_q, split_dq))
        return result[0].reshape(SEQ, DH), result[1].reshape(SEQ, DH)

    whole = lax.map(per_head, (queries, tangent_q, keys, tangent_k, values, tangent_v))
    return whole[0], whole[1]
```

```python
import math

import jax
import jax.numpy as jnp
from jax import lax
from jax.experimental import pallas as pl
from jax.experimental.pallas import tpu as pltpu
from jax.sharding import PartitionSpec as P

F32, BF16 = jnp.float32, jnp.bfloat16
MESH = pl.DeviceIdType.MESH
B = 128
H = 64
ROWS, STATS = 136, 64
HALVES = ((0, 72), (72, 64))
LOG2E = math.log2(math.e)
LOTS = 47


def split(x):
    high = x.astype(BF16)
    return high, (x - high.astype(F32)).astype(BF16)


def dot(a, b):
    return jnp.dot(a, b, preferred_element_type=F32)


def kernel(
    q_ref, k_ref, v_ref, dq_ref, dk_ref, dv_ref, num_out, tan_out,
    q_in, k_in, qt, kb, vt, num, tan, num_in, tan_in, own_sem, send_sem, recv_sem,
):
    pb, ka = lax.axis_index("pb"), lax.axis_index("ka")
    z, core = pb // 2, pb % 2
    x, y = ka // 4, ka % 4
    x_up = {"ka": ((x + 1) % 4) * 4 + y, "pb": pb}
    x_down = {"ka": ((x + 3) % 4) * 4 + y, "pb": pb}
    z_up = {"ka": ka, "pb": ((z + 1) % 4) * 2 + core}
    z_down = {"ka": ka, "pb": ((z + 3) % 4) * 2 + core}
    q_pair = {"ka": x * 4 + y + 1 - 2 * (y % 2), "pb": pb}
    k_pair = {"ka": x * 4 + 3 - y, "pb": pb}
    twin = {"ka": ka, "pb": z * 2 + 1 - core}

    for src, dst in (
        (q_ref, q_in.at[0, 0]), (dq_ref, q_in.at[0, 1]), (k_ref, k_in.at[0, 0, 0]),
        (dk_ref, k_in.at[0, 0, 1]), (v_ref, k_in.at[0, 0, 2]), (dv_ref, k_in.at[0, 0, 3]),
    ):
        pltpu.make_async_copy(src.at[0], dst, own_sem).start()
    barrier = pltpu.get_barrier_semaphore()
    peers = (x_up, x_down, z_up, z_down, q_pair, k_pair, twin)
    for peer in peers:
        pl.semaphore_signal(barrier, inc=1, device_id=peer, device_id_type=MESH)

    lots = {}

    def message(lot, group, src, dst, peer):
        n = lots.setdefault(lot, len(lots))
        return pltpu.make_async_remote_copy(
            src_ref=src, dst_ref=dst, send_sem=send_sem.at[group], recv_sem=recv_sem.at[n],
            device_id=peer, device_id_type=MESH,
        )

    def arrive(lot, size):
        pltpu.make_async_remote_copy(
            src_ref=size, dst_ref=size, send_sem=send_sem.at[0], recv_sem=recv_sem.at[lots[lot]],
            device_id=twin, device_id_type=MESH,
        ).wait_recv()

    def arrays(lot, count, rows=B):
        arrive(lot, k_in.at[:count, 0, 0, :rows])

    def begin(*copies):
        for copy in copies:
            copy.start()

    def q_message(a, src, dst, peer, lot=None):
        return message(lot or ("q", dst, a), 0, q_in.at[src, a], q_in.at[dst, a], peer)

    q1, q2, q3 = ((0, 0, 1, x_up), (0, 0, 2, x_down), (0, 0, 3, q_pair))
    qm = {
        (1, 0): q_message(*q1), (1, 1): q_message(1, 0, 1, x_up),
        (2, 0): q_message(*q2, "q near"), (2, 1): q_message(1, 0, 2, x_down),
        (3, 0): q_message(*q3), (3, 1): q_message(1, 0, 3, q_pair, "q near"),
        (4, 0): q_message(0, 3, 4, x_up, "q far"), (5, 0): q_message(0, 3, 5, x_down),
        (6, 0): q_message(0, 1, 6, x_up, "q far"), (7, 0): q_message(0, 5, 7, x_down, "q far"),
        (4, 1): q_message(1, 1, 4, q_pair, "q far"), (5, 1): q_message(1, 2, 5, q_pair, "q far"),
        (6, 1): q_message(1, 1, 6, x_up), (7, 1): q_message(1, 6, 7, q_pair, "q far"),
    }

    def half(s, c, a, h):
        return k_in.at[s, c, a, pl.ds(h * H, H)]

    near_lots = {
        (1, 2): "v1", (1, 3): "dv1", (2, 2): "v2", (2, 3): "v2",
        (1, 0): "k12", (1, 1): "k12", (2, 0): "k12", (2, 1): "k12",
    }
    near = {
        (s, a, h): message(near_lots[s, a] if h else "k near", 1, half(0, 0, a, h), half(s, 0, a, h), peer)
        for s, peer in ((1, z_up), (2, z_down))
        for a in range(4)
        for h in range(2)
    }

    def k_message(a, src, dst, peer, lot):
        return message(lot, 1, k_in.at[src, 0, a], k_in.at[dst, 0, a], peer)

    km = {}
    for a in range(2):
        km[3, a] = k_message(a, 0, 3, k_pair, ("k3", a))
        km[3, 2 + a] = k_message(2 + a, 0, 3, k_pair, "v3")
        km[4, a] = k_message(a, 3, 4, z_up, "k45")
        km[5, a] = k_message(a, 3, 5, z_down, ("k5", a))
        km[6, a] = k_message(a, 1, 6, z_up, "k67")
        km[7, a] = k_message(a, 5, 7, z_down, "k67")
        v = 2 + a
        km[4, v] = k_message(v, 1, 4, k_pair, "k45")
        km[5, v] = k_message(v, 2, 5, k_pair, "k45")
        km[6, v] = k_message(v, 1 + a, 6, (z_up, z_down)[a], ("v6", a))
        km[7, v] = k_message(v, 6, 7, k_pair, "v7")
    tm = {0: message("t0", 2, k_in.at[0, 0], k_in.at[0, 1], twin)}
    for s in (1, 2):
        for h in range(2):
            rows = pl.ds(h * H, H)
            tm[s, h] = message(("t near", h), 2, k_in.at[s, 0, :, rows], k_in.at[s, 1, :, rows], twin)
    for s in (3, 4, 5, 6, 7):
        for h in range(2):
            pair = pl.ds(2 * h, 2)
            lot = {3: ("t near", 1), 4: "t4", 5: "t56", 6: "t56", 7: "t7"}[s]
            tm[s, h] = message(lot, 2, k_in.at[s, 0, pair], k_in.at[s, 1, pair], twin)

    def whole(lot, group, src, dst, peer):
        return [message(lot, group, src, dst, peer)]

    def halves(lot, group, src, dst, peer):
        return [
            message((lot, at), group, src.at[pl.ds(at, size)], dst.at[pl.ds(at, size)], peer)
            for at, size in HALVES
        ]

    nm = {
        "2": whole("n2", 3, num.at[6], num_in.at[0], x_up),
        "4": halves("n4", 3, num.at[7], num_in.at[1], x_down),
        "3a": whole("n3", 3, num.at[5], num_in.at[2], x_up),
        "3b": halves("n3b", 3, num.at[4], num_in.at[3], x_down),
        "0a": whole("n0", 3, num.at[2], num_in.at[4], x_up),
        "0b": whole("n0", 3, num.at[1], num_in.at[5], x_down),
        "0c": halves("n0c", 3, num.at[3], num_in.at[6], q_pair),
    }
    dm = {
        "6": halves("d6", 4, tan.at[7], tan_in.at[0], q_pair),
        "1": whole("d1", 4, tan.at[4], tan_in.at[1], q_pair),
        "2": whole("d2", 4, tan.at[5], tan_in.at[2], q_pair),
        "0": whole("d0", 4, tan.at[3], tan_in.at[3], q_pair),
        "2a": halves("d2a", 4, tan.at[6], tan_in.at[4], x_up),
        "0a": halves("d0a", 4, tan.at[2], tan_in.at[5], x_up),
        "0b": whole("d0", 4, tan.at[1], tan_in.at[6], x_down),
    }
    assert len(lots) == LOTS, len(lots)

    num[...] = jnp.zeros_like(num)
    tan[...] = jnp.zeros_like(tan)
    for s in range(8):
        num[s, STATS : STATS + 1] = jnp.full((1, B), -1e30, F32)
    own = k_in.at[:6, 0, 0]
    pltpu.make_async_copy(own, own, own_sem).wait()
    pl.semaphore_wait(barrier, len(peers))

    begin(qm[1, 1], qm[2, 1], qm[3, 0])
    for a in range(4):
        begin(km[3, a], near[1, a, 0], near[2, a, 0])
        if a == 0:
            begin(qm[1, 0], qm[2, 0], qm[3, 1], tm[0])
    for a in (2, 3, 0, 1):
        begin(near[1, a, 1], near[2, a, 1])

    scale = B**-0.5 * LOG2E

    def take_q(s):
        for a in range(2):
            high, low = split((q_in[s, a] * scale).T)
            qt[s, 2 * B * a : 2 * B * a + B] = high
            qt[s, 2 * B * a + B : 2 * B * a + 2 * B] = low

    def take_k(at, *parts):
        r = pl.ds(at * B, B)

        def read(a):
            got = [k_in[p[0], p[1], a] if len(p) == 2 else half(*p[:2], a, p[2])[...] for p in parts]
            return got[0] if len(got) == 1 else jnp.concatenate(got, axis=0)

        for a in range(2):
            high, low = split(read(a))
            kb[r, 2 * B * a : 2 * B * a + B] = high
            kb[r, 2 * B * a + B : 2 * B * a + 2 * B] = low
        for a in range(2):
            value = read(2 + a).T
            high, low = split(value * LOG2E if a else value)
            vt[2 * B * a : 2 * B * a + B, r] = high
            vt[2 * B * a + B : 2 * B * a + 2 * B, r] = low

    def step(first, blocks, side):
        r = pl.ds(pl.multiple_of(first * B, B), blocks * B)
        kk, dd = kb[r, : 2 * B], kb[r, 2 * B :]
        khigh = kk[:, :B]
        kd = jnp.concatenate([khigh, dd[:, :B]], axis=1)
        at = [side * 4 + j for j in range(4)]

        def wide(read):
            return jnp.concatenate([read(n) for n in at], axis=1)

        def sums(ref):
            return wide(lambda n: jnp.concatenate([ref[n, :H], ref[n, ROWS - H :]], axis=0))

        def stat(ref, row):
            return wide(lambda n: ref[n, STATS + row : STATS + row + 1])

        def put_sums(ref, value):
            for j, n in enumerate(at):
                ref[n, :H] = value[:H, j * B : (j + 1) * B]
                ref[n, ROWS - H :] = value[H:, j * B : (j + 1) * B]

        def put_stat(ref, row, value):
            for j, n in enumerate(at):
                ref[n, STATS + row : STATS + row + 1] = value[:, j * B : (j + 1) * B]

        qhigh, qlow, dqhigh, dqlow = (
            wide(lambda n: qt[n, m * B : (m + 1) * B]) for m in range(4)
        )
        qq = jnp.concatenate([qhigh, qhigh], axis=0)
        s_ = dot(kk, qq) + dot(khigh, qlow)
        t_ = (
            dot(kk, jnp.concatenate([dqhigh, dqhigh], axis=0))
            + dot(dd, qq)
            + dot(kd, jnp.concatenate([dqlow, qlow], axis=0))
        )
        old = stat(num, 0)
        new = jnp.maximum(old, jnp.max(s_, axis=0, keepdims=True))
        shrink = jnp.exp2(old - new)
        w = jnp.exp2(s_ - new)
        p = w * t_
        put_stat(num, 1, stat(num, 1) * shrink + jnp.sum(w, axis=0, keepdims=True))
        put_stat(tan, 1, stat(tan, 1) * shrink + jnp.sum(p, axis=0, keepdims=True))
        put_stat(num, 0, new)
        put_stat(tan, 0, new)
        whigh, wlow = split(w)
        phigh, plow = split(p)
        vhigh, vlow, dvhigh, dvlow = (vt[n * B : (n + 1) * B, r] for n in range(4))
        n_ = dot(vhigh, whigh) + dot(vlow, whigh) + dot(vhigh, wlow)
        d_ = (
            dot(dvhigh, whigh) + dot(dvlow, whigh) + dot(dvhigh, wlow)
            + dot(vhigh, phigh) + dot(vlow, phigh) + dot(vhigh, plow)
        )
        put_sums(num, sums(num) * shrink + n_)
        put_sums(tan, sums(tan) * shrink + d_)

    def early_0():
        take_q(0)
        take_k(0, (0, 0))
        arrays("t0", 4)
        take_k(1, (0, 1))
        arrays(("q", 1, 1), 1)
        begin(qm[6, 1], qm[4, 1])
        arrays(("q", 2, 1), 1)
        begin(qm[5, 1])
        arrays(("q", 3, 0), 1)
        begin(qm[4, 0], qm[5, 0])
        arrays(("q", 1, 0), 1)
        begin(qm[6, 0])
        arrays("q near", 2)
        arrays(("k3", 0), 1)
        begin(km[4, 0], km[5, 0])
        for s in (1, 2, 3):
            take_q(s)

    def early_1():
        arrays("k near", 4)
        begin(tm[1, 0], tm[2, 0])
        arrays(("k3", 1), 1)
        arrays("v1", 1, H)
        begin(km[6, 2], km[4, 2], km[4, 1], km[5, 1], tm[3, 0])
        take_k(2, (1, 0, 0), (2, 0, 0))
        arrays("dv1", 1, H)
        begin(km[4, 3])
        arrays("v2", 2, H)
        begin(km[6, 3], km[5, 2], km[5, 3])
        arrays(("q", 5, 0), 1)
        begin(qm[7, 0])
        arrays(("q", 6, 1), 1)
        begin(qm[7, 1])
        arrays(("t near", 0), 4)
        take_k(3, (1, 1, 0), (2, 1, 0))

    def early_2():
        arrays("k12", 4, H)
        begin(km[6, 0], km[6, 1], tm[1, 1], tm[2, 1])
        take_k(4, (1, 0, 1), (2, 0, 1))
        arrays("v3", 2)
        begin(tm[3, 1])
        take_k(5, (3, 0))

    def early_3():
        arrays(("t near", 1), 8)
        take_k(6, (1, 1, 1), (2, 1, 1))
        take_k(7, (3, 1))
        arrays(("k5", 0), 1)
        begin(km[7, 0])

    def late_0():
        arrays(("v6", 0), 1)
        begin(km[7, 2])
        arrays(("k5", 1), 1)
        begin(km[7, 1], tm[5, 0])
        arrays("q far", 6)
        for s in (4, 5, 6, 7):
            take_q(s)
        arrays(("v6", 1), 1)
        begin(km[7, 3], tm[6, 1])

    def late_1():
        arrays("k45", 6)
        begin(tm[4, 0], tm[4, 1], tm[5, 1])

    def late_2():
        arrays("k67", 4)
        begin(tm[6, 0], tm[7, 0])
        arrays("t4", 4)
        for n, block in enumerate(((4, 0), (4, 1), (5, 0), (6, 0))):
            take_k(8 + n, block)

    def last_0():
        arrays("v7", 2)
        begin(tm[7, 1])
        arrays("t56", 8)
        take_k(12, (5, 1))
        take_k(13, (6, 1))

    def last_1():
        arrays("t7", 4)
        take_k(14, (7, 0))
        take_k(15, (7, 1))

    def steps(events, first, blocks, side):
        def one(i, carry):
            for n, event in enumerate(events):
                pl.when(i == n)(event)
            step(first + blocks * i, blocks, side)
            return carry

        return one

    lax.fori_loop(0, 4, steps((early_0, early_1, early_2, early_3), 0, 2, 0), 0)
    lax.fori_loop(0, 3, steps((late_0, late_1, late_2), 0, 4, 1), 0)
    lax.fori_loop(0, 2, steps((last_0, last_1), 12, 2, 1), 0)
    begin(*nm["4"], *dm["6"], *nm["2"], *dm["1"], *nm["3a"], *dm["2"])
    lax.fori_loop(0, 2, steps((), 8, 4, 0), 0)

    def add(copies, ref, s, other, then=(), wait=None):
        if wait is not None:
            arrive(*wait)
        factors = None
        for n, (at, size) in enumerate(HALVES):
            if wait is None and n < len(copies):
                copies[n].wait_recv()
            r = pl.ds(at, size)
            if factors is None:
                old, got = ref[s, STATS : STATS + 1], other[STATS : STATS + 1]
                peak = jnp.maximum(old, got)
                factors = jnp.exp2(old - peak), jnp.exp2(got - peak)
            ref[s, r] = ref[s, r] * factors[0] + other[r] * factors[1]
            if n == 0:
                ref[s, STATS : STATS + 1] = peak
            if n >= len(HALVES) - len(then):
                begin(then[n - len(HALVES) + len(then)])

    begin(*dm["0"], *nm["0b"])
    add(dm["6"], tan, 6, tan_in.at[0], dm["2a"])
    add(nm["4"], num, 4, num_in.at[1], nm["3b"])
    add(nm["2"], num, 2, num_in.at[0], nm["0a"])
    add(dm["1"], tan, 1, tan_in.at[1], dm["0b"])
    add(dm["2"], tan, 2, tan_in.at[2])
    add(nm["3a"], num, 3, num_in.at[2])
    add(nm["3b"], num, 3, num_in.at[3], nm["0c"])
    add(dm["2a"], tan, 2, tan_in.at[4], dm["0a"])
    add(nm["0b"], num, 0, num_in.at[5], (), ("n0", num_in.at[:2]))
    add((), num, 0, num_in.at[4])
    add(dm["0"], tan, 0, tan_in.at[3], (), ("d0", tan_in.at[:2]))
    add((), tan, 0, tan_in.at[6])
    add(nm["0c"], num, 0, num_in.at[6])
    add(dm["0a"], tan, 0, tan_in.at[5])
    num_out[...] = num[0]
    tan_out[...] = tan[0]
    for group, size in enumerate((q_in.at[:7], k_in.at[:7, 0], k_in.at[:, 1], num_in, tan_in)):
        pltpu.make_async_remote_copy(
            src_ref=size, dst_ref=size, send_sem=send_sem.at[group], recv_sem=recv_sem.at[0],
            device_id=twin, device_id_type=MESH,
        ).wait_send()


def finish(num, tan, out_ref, tout_ref):
    inverse = 1.0 / num[STATS + 1 : STATS + 2]
    mean = tan[STATS + 1 : STATS + 2] * inverse
    for h, at in enumerate((0, ROWS - H)):
        attended = num[at : at + H] * inverse
        moved = (tan[at : at + H] * inverse - attended * mean) * (1.0 / LOG2E)
        out_ref[0, :, h * H : (h + 1) * H] = attended.T
        tout_ref[0, :, h * H : (h + 1) * H] = moved.T


def body(*args):
    sums = jax.ShapeDtypeStruct((ROWS, B), F32)
    shape = jax.ShapeDtypeStruct((1, B, B), F32)
    vmem = pl.BlockSpec(memory_space=pltpu.VMEM)
    sums = pl.pallas_call(
        kernel,
        out_shape=[sums, sums],
        in_specs=[pl.BlockSpec(memory_space=pltpu.HBM)] * 6,
        out_specs=[vmem, vmem],
        scratch_shapes=[
            pltpu.VMEM((8, 2, B, B), F32),
            pltpu.VMEM((8, 2, 4, B, B), F32),
            pltpu.VMEM((8, 4 * B, B), BF16),
            pltpu.VMEM((16 * B, 4 * B), BF16),
            pltpu.VMEM((4 * B, 16 * B), BF16),
            pltpu.VMEM((8, ROWS, B), F32),
            pltpu.VMEM((8, ROWS, B), F32),
            pltpu.VMEM((7, ROWS, B), F32),
            pltpu.VMEM((7, ROWS, B), F32),
            pltpu.SemaphoreType.DMA,
            pltpu.SemaphoreType.DMA((5,)),
            pltpu.SemaphoreType.DMA((LOTS,)),
        ],
        compiler_params=pltpu.CompilerParams(
            collective_id=0, has_side_effects=True, vmem_limit_bytes=32 << 20
        ),
    )(*(pltpu.with_memory_space_constraint(a, pltpu.HBM) for a in args))
    return pl.pallas_call(
        finish,
        out_shape=[shape, shape],
        in_specs=[vmem, vmem],
        out_specs=[vmem, vmem],
        compiler_params=pltpu.CompilerParams(vmem_limit_bytes=4 << 20),
    )(*sums)


def solution(mesh):
    rows, columns = P(None, ("pb", "ka"), None), P(None, ("ka", "pb"), None)
    return jax.shard_map(
        body,
        mesh=mesh,
        in_specs=(rows, columns, columns, rows, columns, columns),
        out_specs=(rows, rows),
        check_vma=False,
    )
```

```python
import math

import jax
import jax.numpy as jnp
from jax import lax
from jax.experimental import pallas as pl
from jax.experimental.pallas import tpu as pltpu
from jax.sharding import PartitionSpec as P

F32, BF16 = jnp.float32, jnp.bfloat16
MESH = pl.DeviceIdType.MESH
B = 128
H = 64
ROWS, STATS = 136, 64
HALVES = ((0, 72), (72, 64))
LOG2E = math.log2(math.e)
LOTS = 47


def split(x):
    high = x.astype(BF16)
    return high, (x - high.astype(F32)).astype(BF16)


def dot(a, b):
    return jnp.dot(a, b, preferred_element_type=F32)


def kernel(
    q_ref, k_ref, v_ref, dq_ref, dk_ref, dv_ref, num_out, tan_out,
    q_in, k_in, qt, kb, vt, num, tan, num_in, tan_in, own_sem, send_sem, recv_sem,
):
    pb, ka = lax.axis_index("pb"), lax.axis_index("ka")
    z, core = pb // 2, pb % 2
    x, y = ka // 4, ka % 4
    x_up = {"ka": ((x + 1) % 4) * 4 + y, "pb": pb}
    x_down = {"ka": ((x + 3) % 4) * 4 + y, "pb": pb}
    z_up = {"ka": ka, "pb": ((z + 1) % 4) * 2 + core}
    z_down = {"ka": ka, "pb": ((z + 3) % 4) * 2 + core}
    q_pair = {"ka": x * 4 + y + 1 - 2 * (y % 2), "pb": pb}
    k_pair = {"ka": x * 4 + 3 - y, "pb": pb}
    twin = {"ka": ka, "pb": z * 2 + 1 - core}

    for src, dst in (
        (q_ref, q_in.at[0, 0]), (dq_ref, q_in.at[0, 1]), (k_ref, k_in.at[0, 0, 0]),
        (dk_ref, k_in.at[0, 0, 1]), (v_ref, k_in.at[0, 0, 2]), (dv_ref, k_in.at[0, 0, 3]),
    ):
        pltpu.make_async_copy(src.at[0], dst, own_sem).start()
    barrier = pltpu.get_barrier_semaphore()
    peers = (x_up, x_down, z_up, z_down, q_pair, k_pair, twin)
    for peer in peers:
        pl.semaphore_signal(barrier, inc=1, device_id=peer, device_id_type=MESH)

    lots = {}

    def message(lot, group, src, dst, peer):
        n = lots.setdefault(lot, len(lots))
        return pltpu.make_async_remote_copy(
            src_ref=src, dst_ref=dst, send_sem=send_sem.at[group], recv_sem=recv_sem.at[n],
            device_id=peer, device_id_type=MESH,
        )

    def arrive(lot, size):
        pltpu.make_async_remote_copy(
            src_ref=size, dst_ref=size, send_sem=send_sem.at[0], recv_sem=recv_sem.at[lots[lot]],
            device_id=twin, device_id_type=MESH,
        ).wait_recv()

    def arrays(lot, count, rows=B):
        arrive(lot, k_in.at[:count, 0, 0, :rows])

    def begin(*copies):
        for copy in copies:
            copy.start()

    def q_message(a, src, dst, peer, lot=None):
        return message(lot or ("q", dst, a), 0, q_in.at[src, a], q_in.at[dst, a], peer)

    q1, q2, q3 = ((0, 0, 1, x_up), (0, 0, 2, x_down), (0, 0, 3, q_pair))
    qm = {
        (1, 0): q_message(*q1), (1, 1): q_message(1, 0, 1, x_up),
        (2, 0): q_message(*q2, "q near"), (2, 1): q_message(1, 0, 2, x_down),
        (3, 0): q_message(*q3), (3, 1): q_message(1, 0, 3, q_pair, "q near"),
        (4, 0): q_message(0, 3, 4, x_up, "q far"), (5, 0): q_message(0, 3, 5, x_down),
        (6, 0): q_message(0, 1, 6, x_up, "q far"), (7, 0): q_message(0, 5, 7, x_down, "q far"),
        (4, 1): q_message(1, 1, 4, q_pair, "q far"), (5, 1): q_message(1, 2, 5, q_pair, "q far"),
        (6, 1): q_message(1, 1, 6, x_up), (7, 1): q_message(1, 6, 7, q_pair, "q far"),
    }

    def half(s, c, a, h):
        return k_in.at[s, c, a, pl.ds(h * H, H)]

    near_lots = {
        (1, 2): "v1", (1, 3): "dv1", (2, 2): "v2", (2, 3): "v2",
        (1, 0): "k12", (1, 1): "k12", (2, 0): "k12", (2, 1): "k12",
    }
    near = {
        (s, a, h): message(near_lots[s, a] if h else "k near", 1, half(0, 0, a, h), half(s, 0, a, h), peer)
        for s, peer in ((1, z_up), (2, z_down))
        for a in range(4)
        for h in range(2)
    }

    def k_message(a, src, dst, peer, lot):
        return message(lot, 1, k_in.at[src, 0, a], k_in.at[dst, 0, a], peer)

    km = {}
    for a in range(2):
        km[3, a] = k_message(a, 0, 3, k_pair, ("k3", a))
        km[3, 2 + a] = k_message(2 + a, 0, 3, k_pair, "v3")
        km[4, a] = k_message(a, 3, 4, z_up, "k45")
        km[5, a] = k_message(a, 3, 5, z_down, ("k5", a))
        km[6, a] = k_message(a, 1, 6, z_up, "k67")
        km[7, a] = k_message(a, 5, 7, z_down, "k67")
        v = 2 + a
        km[4, v] = k_message(v, 1, 4, k_pair, "k45")
        km[5, v] = k_message(v, 2, 5, k_pair, "k45")
        km[6, v] = k_message(v, 1 + a, 6, (z_up, z_down)[a], ("v6", a))
        km[7, v] = k_message(v, 6, 7, k_pair, "v7")
    tm = {0: message("t0", 2, k_in.at[0, 0], k_in.at[0, 1], twin)}
    for s in (1, 2):
        for h in range(2):
            rows = pl.ds(h * H, H)
            tm[s, h] = message(("t near", h), 2, k_in.at[s, 0, :, rows], k_in.at[s, 1, :, rows], twin)
    for s in (3, 4, 5, 6, 7):
        for h in range(2):
            pair = pl.ds(2 * h, 2)
            lot = {3: ("t near", 1), 4: "t4", 5: "t56", 6: "t56", 7: "t7"}[s]
            tm[s, h] = message(lot, 2, k_in.at[s, 0, pair], k_in.at[s, 1, pair], twin)

    def whole(lot, group, src, dst, peer):
        return [message(lot, group, src, dst, peer)]

    def halves(lot, group, src, dst, peer):
        return [
            message((lot, at), group, src.at[pl.ds(at, size)], dst.at[pl.ds(at, size)], peer)
            for at, size in HALVES
        ]

    nm = {
        "2": whole("n2", 3, num.at[6], num_in.at[0], x_up),
        "4": halves("n4", 3, num.at[7], num_in.at[1], x_down),
        "3a": whole("n3", 3, num.at[5], num_in.at[2], x_up),
        "3b": halves("n3b", 3, num.at[4], num_in.at[3], x_down),
        "0a": whole("n0", 3, num.at[2], num_in.at[4], x_up),
        "0b": whole("n0", 3, num.at[1], num_in.at[5], x_down),
        "0c": halves("n0c", 3, num.at[3], num_in.at[6], q_pair),
    }
    dm = {
        "6": halves("d6", 4, tan.at[7], tan_in.at[0], q_pair),
        "1": whole("d1", 4, tan.at[4], tan_in.at[1], q_pair),
        "2": whole("d2", 4, tan.at[5], tan_in.at[2], q_pair),
        "0": whole("d0", 4, tan.at[3], tan_in.at[3], q_pair),
        "2a": halves("d2a", 4, tan.at[6], tan_in.at[4], x_up),
        "0a": halves("d0a", 4, tan.at[2], tan_in.at[5], x_up),
        "0b": whole("d0", 4, tan.at[1], tan_in.at[6], x_down),
    }
    assert len(lots) == LOTS, len(lots)

    num[...] = jnp.zeros_like(num)
    tan[...] = jnp.zeros_like(tan)
    for s in range(8):
        num[s, STATS : STATS + 1] = jnp.full((1, B), -1e30, F32)
    own = k_in.at[:6, 0, 0]
    pltpu.make_async_copy(own, own, own_sem).wait()
    pl.semaphore_wait(barrier, len(peers))

    begin(qm[1, 1], qm[2, 1], qm[3, 0])
    for a in range(4):
        begin(km[3, a], near[1, a, 0], near[2, a, 0])
        if a == 0:
            begin(qm[1, 0], qm[2, 0], qm[3, 1], tm[0])
    for a in (2, 3, 0, 1):
        begin(near[1, a, 1], near[2, a, 1])

    scale = B**-0.5 * LOG2E

    def take_q(s):
        for a in range(2):
            high, low = split((q_in[s, a] * scale).T)
            qt[s, 2 * B * a : 2 * B * a + B] = high
            qt[s, 2 * B * a + B : 2 * B * a + 2 * B] = low

    def take_k(at, *parts):
        r = pl.ds(at * B, B)

        def read(a):
            got = [k_in[p[0], p[1], a] if len(p) == 2 else half(*p[:2], a, p[2])[...] for p in parts]
            return got[0] if len(got) == 1 else jnp.concatenate(got, axis=0)

        for a in range(2):
            high, low = split(read(a))
            kb[r, 2 * B * a : 2 * B * a + B] = high
            kb[r, 2 * B * a + B : 2 * B * a + 2 * B] = low
        for a in range(2):
            value = read(2 + a).T
            high, low = split(value * LOG2E if a else value)
            vt[2 * B * a : 2 * B * a + B, r] = high
            vt[2 * B * a + B : 2 * B * a + 2 * B, r] = low

    def step(first, blocks, side):
        r = pl.ds(pl.multiple_of(first * B, B), blocks * B)
        kk, dd = kb[r, : 2 * B], kb[r, 2 * B :]
        khigh = kk[:, :B]
        kd = jnp.concatenate([khigh, dd[:, :B]], axis=1)
        at = [side * 4 + j for j in range(4)]

        def wide(read):
            return jnp.concatenate([read(n) for n in at], axis=1)

        def sums(ref):
            return wide(lambda n: jnp.concatenate([ref[n, :H], ref[n, ROWS - H :]], axis=0))

        def stat(ref, row):
            return wide(lambda n: ref[n, STATS + row : STATS + row + 1])

        def put_sums(ref, value):
            for j, n in enumerate(at):
                ref[n, :H] = value[:H, j * B : (j + 1) * B]
                ref[n, ROWS - H :] = value[H:, j * B : (j + 1) * B]

        def put_stat(ref, row, value):
            for j, n in enumerate(at):
                ref[n, STATS + row : STATS + row + 1] = value[:, j * B : (j + 1) * B]

        qhigh, qlow, dqhigh, dqlow = (
            wide(lambda n: qt[n, m * B : (m + 1) * B]) for m in range(4)
        )
        qq = jnp.concatenate([qhigh, qhigh], axis=0)
        s_ = dot(kk, qq) + dot(khigh, qlow)
        t_ = (
            dot(kk, jnp.concatenate([dqhigh, dqhigh], axis=0))
            + dot(dd, qq)
            + dot(kd, jnp.concatenate([dqlow, qlow], axis=0))
        )
        old = stat(num, 0)
        new = jnp.maximum(old, jnp.max(s_, axis=0, keepdims=True))
        shrink = jnp.exp2(old - new)
        w = jnp.exp2(s_ - new)
        p = w * t_
        put_stat(num, 1, stat(num, 1) * shrink + jnp.sum(w, axis=0, keepdims=True))
        put_stat(tan, 1, stat(tan, 1) * shrink + jnp.sum(p, axis=0, keepdims=True))
        put_stat(num, 0, new)
        put_stat(tan, 0, new)
        whigh, wlow = split(w)
        phigh, plow = split(p)
        vhigh, vlow, dvhigh, dvlow = (vt[n * B : (n + 1) * B, r] for n in range(4))
        n_ = dot(vhigh, whigh) + dot(vlow, whigh) + dot(vhigh, wlow)
        d_ = (
            dot(dvhigh, whigh) + dot(dvlow, whigh) + dot(dvhigh, wlow)
            + dot(vhigh, phigh) + dot(vlow, phigh) + dot(vhigh, plow)
        )
        put_sums(num, sums(num) * shrink + n_)
        put_sums(tan, sums(tan) * shrink + d_)

    def early_0():
        take_q(0)
        take_k(0, (0, 0))
        arrays("t0", 4)
        take_k(1, (0, 1))
        arrays(("q", 1, 1), 1)
        begin(qm[6, 1], qm[4, 1])
        arrays(("q", 2, 1), 1)
        begin(qm[5, 1])
        arrays(("q", 3, 0), 1)
        begin(qm[4, 0], qm[5, 0])
        arrays(("q", 1, 0), 1)
        begin(qm[6, 0])
        arrays("q near", 2)
        arrays(("k3", 0), 1)
        begin(km[4, 0], km[5, 0])
        for s in (1, 2, 3):
            take_q(s)

    def early_1():
        arrays("k near", 4)
        begin(tm[1, 0], tm[2, 0])
        arrays(("k3", 1), 1)
        arrays("v1", 1, H)
        begin(km[6, 2], km[4, 2], km[4, 1], km[5, 1], tm[3, 0])
        take_k(2, (1, 0, 0), (2, 0, 0))
        arrays("dv1", 1, H)
        begin(km[4, 3])
        arrays("v2", 2, H)
        begin(km[6, 3], km[5, 2], km[5, 3])
        arrays(("q", 5, 0), 1)
        begin(qm[7, 0])
        arrays(("q", 6, 1), 1)
        begin(qm[7, 1])
        arrays(("t near", 0), 4)
        take_k(3, (1, 1, 0), (2, 1, 0))

    def early_2():
        arrays("k12", 4, H)
        begin(km[6, 0], km[6, 1], tm[1, 1], tm[2, 1])
        take_k(4, (1, 0, 1), (2, 0, 1))
        arrays("v3", 2)
        begin(tm[3, 1])
        take_k(5, (3, 0))

    def early_3():
        arrays(("t near", 1), 8)
        take_k(6, (1, 1, 1), (2, 1, 1))
        take_k(7, (3, 1))
        arrays(("k5", 0), 1)
        begin(km[7, 0])

    def late_0():
        arrays(("v6", 0), 1)
        begin(km[7, 2])
        arrays(("k5", 1), 1)
        begin(km[7, 1], tm[5, 0])
        arrays("q far", 6)
        for s in (4, 5, 6, 7):
            take_q(s)
        arrays(("v6", 1), 1)
        begin(km[7, 3], tm[6, 1])

    def late_1():
        arrays("k45", 6)
        begin(tm[4, 0], tm[4, 1], tm[5, 1])

    def late_2():
        arrays("k67", 4)
        begin(tm[6, 0], tm[7, 0])
        arrays("t4", 4)
        for n, block in enumerate(((4, 0), (4, 1), (5, 0), (6, 0))):
            take_k(8 + n, block)

    def last_0():
        arrays("v7", 2)
        begin(tm[7, 1])
        arrays("t56", 8)
        take_k(12, (5, 1))
        take_k(13, (6, 1))

    def last_1():
        arrays("t7", 4)
        take_k(14, (7, 0))
        take_k(15, (7, 1))

    def steps(events, first, blocks, side):
        def one(i, carry):
            for n, event in enumerate(events):
                pl.when(i == n)(event)
            step(first + blocks * i, blocks, side)
            return carry

        return one

    lax.fori_loop(0, 4, steps((early_0, early_1, early_2, early_3), 0, 2, 0), 0)
    lax.fori_loop(0, 3, steps((late_0, late_1, late_2), 0, 4, 1), 0)
    lax.fori_loop(0, 2, steps((last_0, last_1), 12, 2, 1), 0)
    begin(*nm["4"], *dm["6"], *nm["2"], *dm["1"], *nm["3a"], *dm["2"])
    lax.fori_loop(0, 2, steps((), 8, 4, 0), 0)

    def join(ref, s, other):
        old, got = ref[s, STATS : STATS + 1], other[STATS : STATS + 1]
        peak = jnp.maximum(old, got)
        mine, theirs = jnp.exp2(old - peak), jnp.exp2(got - peak)
        for n, (at, size) in enumerate(HALVES):
            r = pl.ds(at, size)
            ref[s, r] = ref[s, r] * mine + other[r] * theirs
            if n == 0:
                ref[s, STATS : STATS + 1] = peak
                yield

    def add(copies, ref, s, other, then=()):
        for copy in copies:
            copy.wait_recv()
        for _ in join(ref, s, other):
            pass
        begin(*then)

    def relay(*chains):
        joins = [join(ref, s, other) for _, ref, s, other, _ in chains]
        for n in range(2):
            for part, (copies, _, _, _, then) in zip(joins, chains):
                copies[n].wait_recv()
                next(part, None)
                begin(*then[n : n + 1])

    begin(*dm["0"])
    relay((dm["6"], tan, 6, tan_in.at[0], dm["2a"]), (nm["4"], num, 4, num_in.at[1], nm["3b"]))
    begin(*nm["0b"])
    add(nm["2"], num, 2, num_in.at[0], nm["0a"])
    add(dm["1"], tan, 1, tan_in.at[1], dm["0b"])
    add(nm["3a"], num, 3, num_in.at[2])
    add(dm["2"], tan, 2, tan_in.at[2])
    relay((dm["2a"], tan, 2, tan_in.at[4], dm["0a"]), (nm["3b"], num, 3, num_in.at[3], nm["0c"]))
    arrive("n0", num_in.at[:2])
    add((), num, 0, num_in.at[5])
    add((), num, 0, num_in.at[4])
    relay((dm["0a"], tan, 0, tan_in.at[5], ()), (nm["0c"], num, 0, num_in.at[6], ()))
    arrive("d0", tan_in.at[:2])
    add((), tan, 0, tan_in.at[3])
    add((), tan, 0, tan_in.at[6])
    num_out[...] = num[0]
    tan_out[...] = tan[0]
    for group, size in enumerate((q_in.at[:7], k_in.at[:7, 0], k_in.at[:, 1], num_in, tan_in)):
        pltpu.make_async_remote_copy(
            src_ref=size, dst_ref=size, send_sem=send_sem.at[group], recv_sem=recv_sem.at[0],
            device_id=twin, device_id_type=MESH,
        ).wait_send()


def finish(num, tan, out_ref, tout_ref):
    inverse = 1.0 / num[STATS + 1 : STATS + 2]
    mean = tan[STATS + 1 : STATS + 2] * inverse
    for h, at in enumerate((0, ROWS - H)):
        attended = num[at : at + H] * inverse
        moved = (tan[at : at + H] * inverse - attended * mean) * (1.0 / LOG2E)
        out_ref[0, :, h * H : (h + 1) * H] = attended.T
        tout_ref[0, :, h * H : (h + 1) * H] = moved.T


def body(*args):
    sums = jax.ShapeDtypeStruct((ROWS, B), F32)
    shape = jax.ShapeDtypeStruct((1, B, B), F32)
    vmem = pl.BlockSpec(memory_space=pltpu.VMEM)
    sums = pl.pallas_call(
        kernel,
        out_shape=[sums, sums],
        in_specs=[pl.BlockSpec(memory_space=pltpu.HBM)] * 6,
        out_specs=[vmem, vmem],
        scratch_shapes=[
            pltpu.VMEM((8, 2, B, B), F32),
            pltpu.VMEM((8, 2, 4, B, B), F32),
            pltpu.VMEM((8, 4 * B, B), BF16),
            pltpu.VMEM((16 * B, 4 * B), BF16),
            pltpu.VMEM((4 * B, 16 * B), BF16),
            pltpu.VMEM((8, ROWS, B), F32),
            pltpu.VMEM((8, ROWS, B), F32),
            pltpu.VMEM((7, ROWS, B), F32),
            pltpu.VMEM((7, ROWS, B), F32),
            pltpu.SemaphoreType.DMA,
            pltpu.SemaphoreType.DMA((5,)),
            pltpu.SemaphoreType.DMA((LOTS,)),
        ],
        compiler_params=pltpu.CompilerParams(
            collective_id=0, has_side_effects=True, vmem_limit_bytes=32 << 20
        ),
    )(*(pltpu.with_memory_space_constraint(a, pltpu.HBM) for a in args))
    return pl.pallas_call(
        finish,
        out_shape=[shape, shape],
        in_specs=[vmem, vmem],
        out_specs=[vmem, vmem],
        compiler_params=pltpu.CompilerParams(vmem_limit_bytes=4 << 20),
    )(*sums)


def solution(mesh):
    rows, columns = P(None, ("pb", "ka"), None), P(None, ("ka", "pb"), None)
    return jax.shard_map(
        body,
        mesh=mesh,
        in_specs=(rows, columns, columns, rows, columns, columns),
        out_specs=(rows, rows),
        check_vma=False,
    )
```

```python
import math

import jax
import jax.numpy as jnp
from jax import lax
from jax.experimental import pallas as pl
from jax.experimental.pallas import tpu as pltpu
from jax.sharding import PartitionSpec as P

F32, BF16 = jnp.float32, jnp.bfloat16
MESH = pl.DeviceIdType.MESH
B = 128
H = 64
ROWS, DATA = 136, 8
PIECES = ((0, 72), (72, 64))
LOG2E = math.log2(math.e)
LOTS = 50


def split(x):
    high = x.astype(BF16)
    return high, (x - high.astype(F32)).astype(BF16)


def dot(a, b):
    return jnp.dot(a, b, preferred_element_type=F32)


def kernel(
    q_ref, k_ref, v_ref, dq_ref, dk_ref, dv_ref, num_out, tan_out,
    q_in, k_in, qt, kb, vt, num, tan, num_in, tan_in, own_sem, send_sem, recv_sem,
):
    pb, ka = lax.axis_index("pb"), lax.axis_index("ka")
    z, core = pb // 2, pb % 2
    x, y = ka // 4, ka % 4
    x_up = {"ka": ((x + 1) % 4) * 4 + y, "pb": pb}
    x_down = {"ka": ((x + 3) % 4) * 4 + y, "pb": pb}
    z_up = {"ka": ka, "pb": ((z + 1) % 4) * 2 + core}
    z_down = {"ka": ka, "pb": ((z + 3) % 4) * 2 + core}
    q_pair = {"ka": x * 4 + y + 1 - 2 * (y % 2), "pb": pb}
    k_pair = {"ka": x * 4 + 3 - y, "pb": pb}
    twin = {"ka": ka, "pb": z * 2 + 1 - core}

    for src, dst in (
        (q_ref, q_in.at[0, 0]), (dq_ref, q_in.at[0, 1]), (k_ref, k_in.at[0, 0, 0]),
        (dk_ref, k_in.at[0, 0, 1]), (v_ref, k_in.at[0, 0, 2]), (dv_ref, k_in.at[0, 0, 3]),
    ):
        pltpu.make_async_copy(src.at[0], dst, own_sem).start()
    barrier = pltpu.get_barrier_semaphore()
    peers = (x_up, x_down, z_up, z_down, q_pair, k_pair, twin)
    for peer in peers:
        pl.semaphore_signal(barrier, inc=1, device_id=peer, device_id_type=MESH)

    lots = {}

    def message(lot, group, src, dst, peer):
        n = lots.setdefault(lot, len(lots))
        return pltpu.make_async_remote_copy(
            src_ref=src, dst_ref=dst, send_sem=send_sem.at[group], recv_sem=recv_sem.at[n],
            device_id=peer, device_id_type=MESH,
        )

    def arrive(lot, size):
        pltpu.make_async_remote_copy(
            src_ref=size, dst_ref=size, send_sem=send_sem.at[0], recv_sem=recv_sem.at[lots[lot]],
            device_id=twin, device_id_type=MESH,
        ).wait_recv()

    def arrays(lot, count, rows=B):
        arrive(lot, k_in.at[:count, 0, 0, :rows])

    def begin(*copies):
        for copy in copies:
            copy.start()

    def q_message(a, src, dst, peer, lot=None):
        return message(lot or ("q", dst, a), 0, q_in.at[src, a], q_in.at[dst, a], peer)

    q1, q2, q3 = ((0, 0, 1, x_up), (0, 0, 2, x_down), (0, 0, 3, q_pair))
    qm = {
        (1, 0): q_message(*q1), (1, 1): q_message(1, 0, 1, x_up),
        (2, 0): q_message(*q2, "q near"), (2, 1): q_message(1, 0, 2, x_down),
        (3, 0): q_message(*q3), (3, 1): q_message(1, 0, 3, q_pair, "q near"),
        (4, 0): q_message(0, 3, 4, x_up, "q far"), (5, 0): q_message(0, 3, 5, x_down),
        (6, 0): q_message(0, 1, 6, x_up, "q far"), (7, 0): q_message(0, 5, 7, x_down, "q 7"),
        (4, 1): q_message(1, 1, 4, q_pair, "q far"), (5, 1): q_message(1, 2, 5, q_pair, "q far"),
        (6, 1): q_message(1, 1, 6, x_up), (7, 1): q_message(1, 6, 7, q_pair, "q 7"),
    }

    def half(s, c, a, h):
        return k_in.at[s, c, a, pl.ds(h * H, H)]

    near_lots = {
        (1, 2): "v1", (1, 3): "dv1", (2, 2): "v2", (2, 3): "v2",
        (1, 0): "k12", (1, 1): "k12", (2, 0): "k12", (2, 1): "k12",
    }
    near = {
        (s, a, h): message(near_lots[s, a] if h else "k near", 1, half(0, 0, a, h), half(s, 0, a, h), peer)
        for s, peer in ((1, z_up), (2, z_down))
        for a in range(4)
        for h in range(2)
    }

    def k_message(a, src, dst, peer, lot):
        return message(lot, 1, k_in.at[src, 0, a], k_in.at[dst, 0, a], peer)

    km = {}
    for a in range(2):
        km[3, a] = k_message(a, 0, 3, k_pair, ("k3", a))
        km[3, 2 + a] = k_message(2 + a, 0, 3, k_pair, "v3")
        km[4, a] = k_message(a, 3, 4, z_up, "k4")
        km[5, a] = k_message(a, 3, 5, z_down, ("k5", a))
        km[6, a] = k_message(a, 1, 6, z_up, "k6")
        km[7, a] = k_message(a, 5, 7, z_down, "k7")
        v = 2 + a
        km[4, v] = k_message(v, 1, 4, k_pair, "k4")
        km[5, v] = k_message(v, 2, 5, k_pair, "v5")
        km[6, v] = k_message(v, 1 + a, 6, (z_up, z_down)[a], ("v6", a))
        km[7, v] = k_message(v, 6, 7, k_pair, "v7")
    tm = {0: message("t0", 2, k_in.at[0, 0], k_in.at[0, 1], twin)}
    for s in (1, 2):
        for h in range(2):
            rows = pl.ds(h * H, H)
            tm[s, h] = message(("t near", h), 2, k_in.at[s, 0, :, rows], k_in.at[s, 1, :, rows], twin)
    for s in (3, 4, 5, 6, 7):
        for h in range(2):
            pair = pl.ds(2 * h, 2)
            lot = {3: ("t near", 1), 4: "t4", 5: "t56", 6: "t56", 7: "t7"}[s]
            tm[s, h] = message(lot, 2, k_in.at[s, 0, pair], k_in.at[s, 1, pair], twin)

    def whole(lot, group, src, dst, peer):
        return [message(lot, group, src, dst, peer)]

    def pieces(lot, group, src, dst, peer):
        return [
            message((lot, at), group, src.at[pl.ds(at, size)], dst.at[pl.ds(at, size)], peer)
            for at, size in PIECES
        ]

    nm = {
        "2": whole("n2", 3, num.at[6], num_in.at[0], x_up),
        "4": pieces("n4", 3, num.at[7], num_in.at[1], x_down),
        "3a": whole("n3", 3, num.at[5], num_in.at[2], x_up),
        "3b": pieces("n3b", 3, num.at[4], num_in.at[3], x_down),
        "0a": whole("n0", 3, num.at[2], num_in.at[4], x_up),
        "0b": whole("n0", 3, num.at[1], num_in.at[5], x_down),
        "0c": pieces("n0c", 3, num.at[3], num_in.at[6], q_pair),
    }
    dm = {
        "6": pieces("d6", 4, tan.at[7], tan_in.at[0], q_pair),
        "1": whole("d1", 4, tan.at[4], tan_in.at[1], q_pair),
        "2": whole("d2", 4, tan.at[5], tan_in.at[2], q_pair),
        "0": whole("d0", 4, tan.at[3], tan_in.at[3], q_pair),
        "2a": pieces("d2a", 4, tan.at[6], tan_in.at[4], x_up),
        "0a": pieces("d0a", 4, tan.at[2], tan_in.at[5], x_up),
        "0b": whole("d0", 4, tan.at[1], tan_in.at[6], x_down),
    }
    assert len(lots) == LOTS, len(lots)

    num[...] = jnp.zeros_like(num)
    tan[...] = jnp.zeros_like(tan)
    for s in range(8):
        num[s, :1] = jnp.full((1, B), -1e30, F32)
    own = k_in.at[:6, 0, 0]
    pltpu.make_async_copy(own, own, own_sem).wait()
    pl.semaphore_wait(barrier, len(peers))

    begin(qm[1, 1], qm[2, 1], qm[3, 0])
    for a in range(4):
        begin(km[3, a], near[1, a, 0], near[2, a, 0])
        if a == 0:
            begin(qm[1, 0], qm[2, 0], qm[3, 1], tm[0])
    for a in (2, 3, 0, 1):
        begin(near[1, a, 1], near[2, a, 1])

    scale = B**-0.5 * LOG2E

    def take_q(s):
        for a in range(2):
            high, low = split((q_in[s, a] * scale).T)
            qt[s, 2 * B * a : 2 * B * a + B] = high
            qt[s, 2 * B * a + B : 2 * B * a + 2 * B] = low

    def take_k(at, *parts):
        r = pl.ds(at * B, B)

        def read(a):
            got = [k_in[p[0], p[1], a] if len(p) == 2 else half(*p[:2], a, p[2])[...] for p in parts]
            return got[0] if len(got) == 1 else jnp.concatenate(got, axis=0)

        for a in range(2):
            high, low = split(read(a))
            kb[r, 2 * B * a : 2 * B * a + B] = high
            kb[r, 2 * B * a + B : 2 * B * a + 2 * B] = low
        for a in range(2):
            value = read(2 + a).T
            high, low = split(value * LOG2E if a else value)
            vt[2 * B * a : 2 * B * a + B, r] = high
            vt[2 * B * a + B : 2 * B * a + 2 * B, r] = low

    def step(first, blocks, side):
        r = pl.ds(pl.multiple_of(first * B, B), blocks * B)
        kk, dd = kb[r, : 2 * B], kb[r, 2 * B :]
        khigh = kk[:, :B]
        kd = jnp.concatenate([khigh, dd[:, :B]], axis=1)
        at = [side * 4 + j for j in range(4)]

        def wide(read):
            return jnp.concatenate([read(n) for n in at], axis=1)

        def sums(ref):
            return wide(lambda n: ref[n, DATA:])

        def stat(ref, row):
            return wide(lambda n: ref[n, row : row + 1])

        def put_sums(ref, value):
            for j, n in enumerate(at):
                ref[n, DATA:] = value[:, j * B : (j + 1) * B]

        def put_stat(ref, row, value):
            for j, n in enumerate(at):
                ref[n, row : row + 1] = value[:, j * B : (j + 1) * B]

        qhigh, qlow, dqhigh, dqlow = (
            wide(lambda n: qt[n, m * B : (m + 1) * B]) for m in range(4)
        )
        qq = jnp.concatenate([qhigh, qhigh], axis=0)
        s_ = dot(kk, qq) + dot(khigh, qlow)
        t_ = (
            dot(kk, jnp.concatenate([dqhigh, dqhigh], axis=0))
            + dot(dd, qq)
            + dot(kd, jnp.concatenate([dqlow, qlow], axis=0))
        )
        old = stat(num, 0)
        new = jnp.maximum(old, jnp.max(s_, axis=0, keepdims=True))
        shrink = jnp.exp2(old - new)
        w = jnp.exp2(s_ - new)
        p = w * t_
        put_stat(num, 1, stat(num, 1) * shrink + jnp.sum(w, axis=0, keepdims=True))
        put_stat(tan, 1, stat(tan, 1) * shrink + jnp.sum(p, axis=0, keepdims=True))
        put_stat(num, 0, new)
        put_stat(tan, 0, new)
        whigh, wlow = split(w)
        phigh, plow = split(p)
        vhigh, vlow, dvhigh, dvlow = (vt[n * B : (n + 1) * B, r] for n in range(4))
        n_ = dot(vhigh, whigh) + dot(vlow, whigh) + dot(vhigh, wlow)
        d_ = (
            dot(dvhigh, whigh) + dot(dvlow, whigh) + dot(dvhigh, wlow)
            + dot(vhigh, phigh) + dot(vlow, phigh) + dot(vhigh, plow)
        )
        put_sums(num, sums(num) * shrink + n_)
        put_sums(tan, sums(tan) * shrink + d_)

    def early_0():
        take_q(0)
        take_k(0, (0, 0))
        arrays("t0", 4)
        take_k(1, (0, 1))
        arrays(("q", 1, 1), 1)
        begin(qm[6, 1], qm[4, 1])
        arrays(("q", 2, 1), 1)
        begin(qm[5, 1])
        arrays(("q", 3, 0), 1)
        begin(qm[4, 0], qm[5, 0])
        arrays(("q", 1, 0), 1)
        begin(qm[6, 0])
        arrays("q near", 2)
        arrays(("k3", 0), 1)
        begin(km[4, 0], km[5, 0])
        for s in (1, 2, 3):
            take_q(s)

    def early_1():
        arrays("k near", 4)
        begin(tm[1, 0], tm[2, 0])
        arrays(("k3", 1), 1)
        arrays("v1", 1, H)
        begin(km[6, 2], km[4, 2], km[4, 1], km[5, 1], tm[3, 0])
        take_k(2, (1, 0, 0), (2, 0, 0))
        arrays("dv1", 1, H)
        begin(km[4, 3])
        arrays("v2", 2, H)
        begin(km[6, 3], km[5, 2], km[5, 3])
        arrays(("q", 5, 0), 1)
        begin(qm[7, 0])
        arrays(("q", 6, 1), 1)
        begin(qm[7, 1])
        arrays(("t near", 0), 4)
        take_k(3, (1, 1, 0), (2, 1, 0))

    def early_2():
        arrays("k12", 4, H)
        begin(km[6, 0], km[6, 1], tm[1, 1], tm[2, 1])
        take_k(4, (1, 0, 1), (2, 0, 1))
        arrays("v3", 2)
        begin(tm[3, 1])
        take_k(5, (3, 0))

    def early_3():
        arrays(("t near", 1), 8)
        take_k(6, (1, 1, 1), (2, 1, 1))
        take_k(7, (3, 1))
        arrays(("k5", 0), 1)
        begin(km[7, 0])

    def late_0():
        arrays(("v6", 0), 1)
        begin(km[7, 2])
        arrays("q far", 4)
        for s in (4, 5, 6):
            take_q(s)
        arrays(("k5", 1), 1)
        begin(km[7, 1], tm[5, 0])
        arrays("q 7", 2)
        take_q(7)
        arrays(("v6", 1), 1)
        begin(km[7, 3], tm[6, 1])

    def late_1():
        arrays("k4", 4)
        begin(tm[4, 0], tm[4, 1])

    def late_2():
        arrays("v5", 2)
        begin(tm[5, 1])
        arrays("k6", 2)
        begin(tm[6, 0])
        arrays("t4", 4)
        for n, block in enumerate(((4, 0), (4, 1), (5, 0), (6, 0))):
            take_k(8 + n, block)

    def last_0():
        arrays("k7", 2)
        begin(tm[7, 0])
        arrays("v7", 2)
        begin(tm[7, 1])
        arrays("t56", 8)
        take_k(12, (5, 1))
        take_k(13, (6, 1))

    def last_1():
        arrays("t7", 4)
        take_k(14, (7, 0))
        take_k(15, (7, 1))

    def steps(events, first, blocks, side):
        def one(i, carry):
            for n, event in enumerate(events):
                pl.when(i == n)(event)
            step(first + blocks * i, blocks, side)
            return carry

        return one

    lax.fori_loop(0, 4, steps((early_0, early_1, early_2, early_3), 0, 2, 0), 0)
    lax.fori_loop(0, 3, steps((late_0, late_1, late_2), 0, 4, 1), 0)
    lax.fori_loop(0, 2, steps((last_0, last_1), 12, 2, 1), 0)
    begin(*nm["4"], *dm["6"], *nm["2"], *dm["1"], *nm["3a"], *dm["2"])
    lax.fori_loop(0, 2, steps((), 8, 4, 0), 0)

    def join(ref, s, other):
        old, got = ref[s, :1], other[:1]
        peak = jnp.maximum(old, got)
        mine, theirs = jnp.exp2(old - peak), jnp.exp2(got - peak)
        for n, (at, size) in enumerate(PIECES):
            r = pl.ds(at, size)
            ref[s, r] = ref[s, r] * mine + other[r] * theirs
            if n == 0:
                ref[s, :1] = peak
            yield

    def add(copies, ref, s, other, then=()):
        for copy in copies:
            copy.wait_recv()
        for _ in join(ref, s, other):
            pass
        begin(*then)

    def relay(*chains):
        joins = [join(ref, s, other) for _, ref, s, other, _ in chains]
        for n in range(len(PIECES)):
            for part, (copies, _, _, _, then) in zip(joins, chains):
                copies[n].wait_recv()
                next(part, None)
                begin(*then[n : n + 1])

    begin(*dm["0"])
    relay((dm["6"], tan, 6, tan_in.at[0], dm["2a"]), (nm["4"], num, 4, num_in.at[1], nm["3b"]))
    begin(*nm["0b"])
    add(nm["2"], num, 2, num_in.at[0], nm["0a"])
    add(dm["1"], tan, 1, tan_in.at[1], dm["0b"])
    add(nm["3a"], num, 3, num_in.at[2])
    add(dm["2"], tan, 2, tan_in.at[2])
    relay((dm["2a"], tan, 2, tan_in.at[4], dm["0a"]), (nm["3b"], num, 3, num_in.at[3], nm["0c"]))
    arrive("n0", num_in.at[:2])
    add((), num, 0, num_in.at[5])
    add((), num, 0, num_in.at[4])
    relay((dm["0a"], tan, 0, tan_in.at[5], ()), (nm["0c"], num, 0, num_in.at[6], ()))
    arrive("d0", tan_in.at[:2])
    add((), tan, 0, tan_in.at[3])
    add((), tan, 0, tan_in.at[6])
    num_out[...] = num[0]
    tan_out[...] = tan[0]
    for group, size in enumerate((q_in.at[:7], k_in.at[:7, 0], k_in.at[:, 1], num_in, tan_in)):
        pltpu.make_async_remote_copy(
            src_ref=size, dst_ref=size, send_sem=send_sem.at[group], recv_sem=recv_sem.at[0],
            device_id=twin, device_id_type=MESH,
        ).wait_send()


def finish(num, tan, out_ref, tout_ref):
    inverse = 1.0 / num[1:2]
    attended = num[DATA:] * inverse
    moved = (tan[DATA:] * inverse - attended * (tan[1:2] * inverse)) * (1.0 / LOG2E)
    out_ref[0] = attended.T
    tout_ref[0] = moved.T


def body(*args):
    sums = jax.ShapeDtypeStruct((ROWS, B), F32)
    shape = jax.ShapeDtypeStruct((1, B, B), F32)
    vmem = pl.BlockSpec(memory_space=pltpu.VMEM)
    sums = pl.pallas_call(
        kernel,
        out_shape=[sums, sums],
        in_specs=[pl.BlockSpec(memory_space=pltpu.HBM)] * 6,
        out_specs=[vmem, vmem],
        scratch_shapes=[
            pltpu.VMEM((8, 2, B, B), F32),
            pltpu.VMEM((8, 2, 4, B, B), F32),
            pltpu.VMEM((8, 4 * B, B), BF16),
            pltpu.VMEM((16 * B, 4 * B), BF16),
            pltpu.VMEM((4 * B, 16 * B), BF16),
            pltpu.VMEM((8, ROWS, B), F32),
            pltpu.VMEM((8, ROWS, B), F32),
            pltpu.VMEM((7, ROWS, B), F32),
            pltpu.VMEM((7, ROWS, B), F32),
            pltpu.SemaphoreType.DMA,
            pltpu.SemaphoreType.DMA((5,)),
            pltpu.SemaphoreType.DMA((LOTS,)),
        ],
        compiler_params=pltpu.CompilerParams(
            collective_id=0, has_side_effects=True, vmem_limit_bytes=32 << 20
        ),
    )(*(pltpu.with_memory_space_constraint(a, pltpu.HBM) for a in args))
    return pl.pallas_call(
        finish,
        out_shape=[shape, shape],
        in_specs=[vmem, vmem],
        out_specs=[vmem, vmem],
        compiler_params=pltpu.CompilerParams(vmem_limit_bytes=4 << 20),
    )(*sums)


def solution(mesh):
    rows, columns = P(None, ("pb", "ka"), None), P(None, ("ka", "pb"), None)
    return jax.shard_map(
        body,
        mesh=mesh,
        in_specs=(rows, columns, columns, rows, columns, columns),
        out_specs=(rows, rows),
        check_vma=False,
    )
```

```python
import math

import jax
import jax.numpy as jnp
from jax import lax
from jax.experimental import pallas as pl
from jax.experimental.pallas import tpu as pltpu
from jax.sharding import PartitionSpec as P

F32, BF16 = jnp.float32, jnp.bfloat16
MESH = pl.DeviceIdType.MESH
B = 128
H = 64
ROWS, DATA = 136, 8
PIECES = ((0, 72), (72, 64))
LOG2E = math.log2(math.e)
LOTS = 50


def split(x):
    high = x.astype(BF16)
    return high, (x - high.astype(F32)).astype(BF16)


def dot(a, b):
    return jnp.dot(a, b, preferred_element_type=F32)


def kernel(
    q_ref, k_ref, v_ref, dq_ref, dk_ref, dv_ref, num_out, tan_out,
    q_in, k_in, qt, kb, vt, num, tan, num_in, tan_in, own_sem, send_sem, recv_sem,
):
    pb, ka = lax.axis_index("pb"), lax.axis_index("ka")
    z, core = pb // 2, pb % 2
    x, y = ka // 4, ka % 4
    x_up = {"ka": ((x + 1) % 4) * 4 + y, "pb": pb}
    x_down = {"ka": ((x + 3) % 4) * 4 + y, "pb": pb}
    z_up = {"ka": ka, "pb": ((z + 1) % 4) * 2 + core}
    z_down = {"ka": ka, "pb": ((z + 3) % 4) * 2 + core}
    q_pair = {"ka": x * 4 + y + 1 - 2 * (y % 2), "pb": pb}
    k_pair = {"ka": x * 4 + 3 - y, "pb": pb}
    twin = {"ka": ka, "pb": z * 2 + 1 - core}

    for src, dst in (
        (q_ref, q_in.at[0, 0]), (dq_ref, q_in.at[0, 1]), (k_ref, k_in.at[0, 0, 0]),
        (dk_ref, k_in.at[0, 0, 1]), (v_ref, k_in.at[0, 0, 2]), (dv_ref, k_in.at[0, 0, 3]),
    ):
        pltpu.make_async_copy(src.at[0], dst, own_sem).start()
    barrier = pltpu.get_barrier_semaphore()
    peers = (x_up, x_down, z_up, z_down, q_pair, k_pair, twin)
    for peer in peers:
        pl.semaphore_signal(barrier, inc=1, device_id=peer, device_id_type=MESH)

    lots = {}

    def message(lot, group, src, dst, peer):
        n = lots.setdefault(lot, len(lots))
        return pltpu.make_async_remote_copy(
            src_ref=src, dst_ref=dst, send_sem=send_sem.at[group], recv_sem=recv_sem.at[n],
            device_id=peer, device_id_type=MESH,
        )

    def arrive(lot, size):
        pltpu.make_async_remote_copy(
            src_ref=size, dst_ref=size, send_sem=send_sem.at[0], recv_sem=recv_sem.at[lots[lot]],
            device_id=twin, device_id_type=MESH,
        ).wait_recv()

    def arrays(lot, count, rows=B):
        arrive(lot, k_in.at[:count, 0, 0, :rows])

    def begin(*copies):
        for copy in copies:
            copy.start()

    def q_message(a, src, dst, peer, lot=None):
        return message(lot or ("q", dst, a), 0, q_in.at[src, a], q_in.at[dst, a], peer)

    q1, q2, q3 = ((0, 0, 1, x_up), (0, 0, 2, x_down), (0, 0, 3, q_pair))
    qm = {
        (1, 0): q_message(*q1), (1, 1): q_message(1, 0, 1, x_up),
        (2, 0): q_message(*q2, "q near"), (2, 1): q_message(1, 0, 2, x_down),
        (3, 0): q_message(*q3), (3, 1): q_message(1, 0, 3, q_pair, "q near"),
        (4, 0): q_message(0, 3, 4, x_up, "q far"), (5, 0): q_message(0, 3, 5, x_down),
        (6, 0): q_message(0, 1, 6, x_up, "q far"), (7, 0): q_message(0, 5, 7, x_down, "q 7"),
        (4, 1): q_message(1, 1, 4, q_pair, "q far"), (5, 1): q_message(1, 2, 5, q_pair, "q far"),
        (6, 1): q_message(1, 1, 6, x_up), (7, 1): q_message(1, 6, 7, q_pair, "q 7"),
    }

    def half(s, c, a, h):
        return k_in.at[s, c, a, pl.ds(h * H, H)]

    near_lots = {
        (1, 2): "v1", (1, 3): "dv1", (2, 2): "v2", (2, 3): "v2",
        (1, 0): "k12", (1, 1): "k12", (2, 0): "k12", (2, 1): "k12",
    }
    near = {
        (s, a, h): message(near_lots[s, a] if h else "k near", 1, half(0, 0, a, h), half(s, 0, a, h), peer)
        for s, peer in ((1, z_up), (2, z_down))
        for a in range(4)
        for h in range(2)
    }

    def k_message(a, src, dst, peer, lot):
        return message(lot, 1, k_in.at[src, 0, a], k_in.at[dst, 0, a], peer)

    km = {}
    for a in range(2):
        km[3, a] = k_message(a, 0, 3, k_pair, ("k3", a))
        km[3, 2 + a] = k_message(2 + a, 0, 3, k_pair, "v3")
        km[4, a] = k_message(a, 3, 4, z_up, "k4")
        km[5, a] = k_message(a, 3, 5, z_down, ("k5", a))
        km[6, a] = k_message(a, 1, 6, z_up, "k6")
        km[7, a] = k_message(a, 5, 7, z_down, "k7")
        v = 2 + a
        km[4, v] = k_message(v, 1, 4, k_pair, "k4")
        km[5, v] = k_message(v, 2, 5, k_pair, "v5")
        km[6, v] = k_message(v, 1 + a, 6, (z_up, z_down)[a], ("v6", a))
        km[7, v] = k_message(v, 6, 7, k_pair, "v7")
    tm = {0: message("t0", 2, k_in.at[0, 0], k_in.at[0, 1], twin)}
    for s in (1, 2):
        for h in range(2):
            rows = pl.ds(h * H, H)
            tm[s, h] = message(("t near", h), 2, k_in.at[s, 0, :, rows], k_in.at[s, 1, :, rows], twin)
    for s in (3, 4, 5, 6, 7):
        for h in range(2):
            pair = pl.ds(2 * h, 2)
            lot = {3: ("t near", 1), 4: "t4", 5: "t56", 6: "t56", 7: "t7"}[s]
            tm[s, h] = message(lot, 2, k_in.at[s, 0, pair], k_in.at[s, 1, pair], twin)

    def whole(lot, group, src, dst, peer):
        return [message(lot, group, src, dst, peer)]

    def pieces(lot, group, src, dst, peer):
        return [
            message((lot, at), group, src.at[pl.ds(at, size)], dst.at[pl.ds(at, size)], peer)
            for at, size in PIECES
        ]

    nm = {
        "2": whole("n2", 3, num.at[6], num_in.at[0], x_up),
        "4": pieces("n4", 3, num.at[7], num_in.at[1], x_down),
        "3a": whole("n3", 3, num.at[5], num_in.at[2], x_up),
        "3b": pieces("n3b", 3, num.at[4], num_in.at[3], x_down),
        "0a": whole("n0", 3, num.at[2], num_in.at[4], x_up),
        "0b": whole("n0", 3, num.at[1], num_in.at[5], x_down),
        "0c": pieces("n0c", 3, num.at[3], num_in.at[6], q_pair),
    }
    dm = {
        "6": pieces("d6", 4, tan.at[7], tan_in.at[0], q_pair),
        "1": whole("d1", 4, tan.at[4], tan_in.at[1], q_pair),
        "2": whole("d2", 4, tan.at[5], tan_in.at[2], q_pair),
        "0": whole("d0", 4, tan.at[3], tan_in.at[3], q_pair),
        "2a": pieces("d2a", 4, tan.at[6], tan_in.at[4], x_up),
        "0a": pieces("d0a", 4, tan.at[2], tan_in.at[5], x_up),
        "0b": whole("d0", 4, tan.at[1], tan_in.at[6], x_down),
    }
    assert len(lots) == LOTS, len(lots)

    num[...] = jnp.zeros_like(num)
    tan[...] = jnp.zeros_like(tan)
    for s in range(8):
        num[s, :1] = jnp.full((1, B), -1e30, F32)
    own = k_in.at[:6, 0, 0]
    pltpu.make_async_copy(own, own, own_sem).wait()
    pl.semaphore_wait(barrier, len(peers))

    begin(qm[1, 1], qm[2, 1], qm[3, 0])
    for a in range(4):
        begin(km[3, a], near[1, a, 0], near[2, a, 0])
        if a == 0:
            begin(qm[1, 0], qm[2, 0], qm[3, 1], tm[0])
    for a in (2, 3, 0, 1):
        begin(near[1, a, 1], near[2, a, 1])

    scale = B**-0.5 * LOG2E

    def take_q(s):
        for a in range(2):
            high, low = split((q_in[s, a] * scale).T)
            qt[s, 2 * B * a : 2 * B * a + B] = high
            qt[s, 2 * B * a + B : 2 * B * a + 2 * B] = low

    def take_k(at, *parts):
        r = pl.ds(at * B, B)

        def read(a):
            got = [k_in[p[0], p[1], a] if len(p) == 2 else half(*p[:2], a, p[2])[...] for p in parts]
            return got[0] if len(got) == 1 else jnp.concatenate(got, axis=0)

        for a in range(2):
            high, low = split(read(a))
            kb[r, 2 * B * a : 2 * B * a + B] = high
            kb[r, 2 * B * a + B : 2 * B * a + 2 * B] = low
        for a in range(2):
            value = read(2 + a).T
            high, low = split(value * LOG2E if a else value)
            vt[2 * B * a : 2 * B * a + B, r] = high
            vt[2 * B * a + B : 2 * B * a + 2 * B, r] = low

    def step(first, blocks, side):
        r = pl.ds(pl.multiple_of(first * B, B), blocks * B)
        kk, dd = kb[r, : 2 * B], kb[r, 2 * B :]
        khigh = kk[:, :B]
        kd = jnp.concatenate([khigh, dd[:, :B]], axis=1)
        at = [side * 4 + j for j in range(4)]

        def wide(read):
            return jnp.concatenate([read(n) for n in at], axis=1)

        def sums(ref):
            return wide(lambda n: ref[n, DATA:])

        def stat(ref, row):
            return wide(lambda n: ref[n, row : row + 1])

        def put_sums(ref, value):
            for j, n in enumerate(at):
                ref[n, DATA:] = value[:, j * B : (j + 1) * B]

        def put_stat(ref, row, value):
            for j, n in enumerate(at):
                ref[n, row : row + 1] = value[:, j * B : (j + 1) * B]

        qhigh, qlow, dqhigh, dqlow = (
            wide(lambda n: qt[n, m * B : (m + 1) * B]) for m in range(4)
        )
        qq = jnp.concatenate([qhigh, qhigh], axis=0)
        s_ = dot(kk, qq) + dot(khigh, qlow)
        t_ = (
            dot(kk, jnp.concatenate([dqhigh, dqhigh], axis=0))
            + dot(dd, qq)
            + dot(kd, jnp.concatenate([dqlow, qlow], axis=0))
        )
        old = stat(num, 0)
        new = jnp.maximum(old, jnp.max(s_, axis=0, keepdims=True))
        shrink = jnp.exp2(old - new)
        w = jnp.exp2(s_ - new)
        p = w * t_
        put_stat(num, 1, stat(num, 1) * shrink + jnp.sum(w, axis=0, keepdims=True))
        put_stat(tan, 1, stat(tan, 1) * shrink + jnp.sum(p, axis=0, keepdims=True))
        put_stat(num, 0, new)
        put_stat(tan, 0, new)
        whigh, wlow = split(w)
        phigh, plow = split(p)
        vhigh, vlow, dvhigh, dvlow = (vt[n * B : (n + 1) * B, r] for n in range(4))
        n_ = dot(vhigh, whigh) + dot(vlow, whigh) + dot(vhigh, wlow)
        d_ = (
            dot(dvhigh, whigh) + dot(dvlow, whigh) + dot(dvhigh, wlow)
            + dot(vhigh, phigh) + dot(vlow, phigh) + dot(vhigh, plow)
        )
        put_sums(num, sums(num) * shrink + n_)
        put_sums(tan, sums(tan) * shrink + d_)

    def early_0():
        take_q(0)
        take_k(0, (0, 0))
        arrays("t0", 4)
        take_k(1, (0, 1))
        arrays(("q", 1, 1), 1)
        begin(qm[6, 1], qm[4, 1])
        arrays(("q", 2, 1), 1)
        begin(qm[5, 1])
        arrays(("q", 3, 0), 1)
        begin(qm[4, 0], qm[5, 0])
        arrays(("q", 1, 0), 1)
        begin(qm[6, 0])
        arrays("q near", 2)
        arrays(("k3", 0), 1)
        begin(km[4, 0], km[5, 0])
        for s in (1, 2, 3):
            take_q(s)

    def early_1():
        arrays("k near", 4)
        begin(tm[1, 0], tm[2, 0])
        arrays(("k3", 1), 1)
        arrays("v1", 1, H)
        begin(km[6, 2], km[4, 2], km[4, 1], km[5, 1], tm[3, 0])
        take_k(2, (1, 0, 0), (2, 0, 0))
        arrays("dv1", 1, H)
        begin(km[4, 3])
        arrays("v2", 2, H)
        begin(km[6, 3], km[5, 2], km[5, 3])
        arrays(("q", 5, 0), 1)
        begin(qm[7, 0])
        arrays(("q", 6, 1), 1)
        begin(qm[7, 1])
        arrays(("t near", 0), 4)
        take_k(3, (1, 1, 0), (2, 1, 0))

    def early_2():
        arrays("k12", 4, H)
        begin(km[6, 0], km[6, 1], tm[1, 1], tm[2, 1])
        take_k(4, (1, 0, 1), (2, 0, 1))
        arrays("v3", 2)
        begin(tm[3, 1])
        take_k(5, (3, 0))

    def early_3():
        arrays(("t near", 1), 8)
        take_k(6, (1, 1, 1), (2, 1, 1))
        take_k(7, (3, 1))
        arrays(("k5", 0), 1)
        begin(km[7, 0])

    def late_0():
        arrays(("v6", 0), 1)
        begin(km[7, 2])
        arrays("q far", 4)
        for s in (4, 5, 6):
            take_q(s)
        arrays(("k5", 1), 1)
        begin(km[7, 1], tm[5, 0])
        arrays("q 7", 2)
        take_q(7)
        arrays(("v6", 1), 1)
        begin(km[7, 3], tm[6, 1])

    def late_1():
        arrays("k4", 4)
        begin(tm[4, 0], tm[4, 1])

    def late_2():
        arrays("v5", 2)
        begin(tm[5, 1])
        arrays("k6", 2)
        begin(tm[6, 0])
        arrays("t4", 4)
        for n, block in enumerate(((4, 0), (4, 1), (5, 0), (6, 0))):
            take_k(8 + n, block)

    def last_0():
        arrays("k7", 2)
        begin(tm[7, 0])
        arrays("v7", 2)
        begin(tm[7, 1])
        arrays("t56", 8)
        take_k(12, (5, 1))
        take_k(13, (6, 1))

    def last_1():
        arrays("t7", 4)
        take_k(14, (7, 0))
        take_k(15, (7, 1))

    def steps(events, first, blocks, side):
        def one(i, carry):
            for n, event in enumerate(events):
                pl.when(i == n)(event)
            step(first + blocks * i, blocks, side)
            return carry

        return one

    lax.fori_loop(0, 4, steps((early_0, early_1, early_2, early_3), 0, 2, 0), 0)
    lax.fori_loop(0, 3, steps((late_0, late_1, late_2), 0, 4, 1), 0)
    lax.fori_loop(0, 2, steps((last_0, last_1), 12, 2, 1), 0)
    begin(*nm["4"], *dm["6"], *nm["2"], *dm["1"], *nm["3a"], *dm["2"])
    lax.fori_loop(0, 2, steps((), 8, 4, 0), 0)

    def join(ref, s, other):
        old, got = ref[s, :1], other[:1]
        peak = jnp.maximum(old, got)
        mine, theirs = jnp.exp2(old - peak), jnp.exp2(got - peak)
        for n, (at, size) in enumerate(PIECES):
            r = pl.ds(at, size)
            ref[s, r] = ref[s, r] * mine + other[r] * theirs
            if n == 0:
                ref[s, :1] = peak
            yield

    def add(copies, ref, s, other, then=()):
        for copy in copies:
            copy.wait_recv()
        for _ in join(ref, s, other):
            pass
        begin(*then)

    def relay(*chains):
        joins = [join(ref, s, other) for _, ref, s, other, _ in chains]
        for n in range(len(PIECES)):
            for part, (copies, _, _, _, then) in zip(joins, chains):
                copies[n].wait_recv()
                next(part, None)
                begin(*then[n : n + 1])

    begin(*dm["0"])
    relay((dm["6"], tan, 6, tan_in.at[0], dm["2a"]), (nm["4"], num, 4, num_in.at[1], nm["3b"]))
    begin(*nm["0b"])
    add(dm["1"], tan, 1, tan_in.at[1], dm["0b"])
    add(nm["2"], num, 2, num_in.at[0], nm["0a"])
    add(nm["3a"], num, 3, num_in.at[2])
    add(dm["2"], tan, 2, tan_in.at[2])
    relay((dm["2a"], tan, 2, tan_in.at[4], dm["0a"]), (nm["3b"], num, 3, num_in.at[3], nm["0c"]))
    arrive("n0", num_in.at[:2])
    add((), num, 0, num_in.at[5])
    add((), num, 0, num_in.at[4])
    relay((dm["0a"], tan, 0, tan_in.at[5], ()), (nm["0c"], num, 0, num_in.at[6], ()))
    arrive("d0", tan_in.at[:2])
    add((), tan, 0, tan_in.at[3])
    add((), tan, 0, tan_in.at[6])
    num_out[...] = num[0]
    tan_out[...] = tan[0]
    for group, size in enumerate((q_in.at[:7], k_in.at[:7, 0], k_in.at[:, 1], num_in, tan_in)):
        pltpu.make_async_remote_copy(
            src_ref=size, dst_ref=size, send_sem=send_sem.at[group], recv_sem=recv_sem.at[0],
            device_id=twin, device_id_type=MESH,
        ).wait_send()


def finish(num, tan, out_ref, tout_ref):
    inverse = 1.0 / num[1:2]
    attended = num[DATA:] * inverse
    moved = (tan[DATA:] * inverse - attended * (tan[1:2] * inverse)) * (1.0 / LOG2E)
    out_ref[0] = attended.T
    tout_ref[0] = moved.T


def body(*args):
    sums = jax.ShapeDtypeStruct((ROWS, B), F32)
    shape = jax.ShapeDtypeStruct((1, B, B), F32)
    vmem = pl.BlockSpec(memory_space=pltpu.VMEM)
    sums = pl.pallas_call(
        kernel,
        out_shape=[sums, sums],
        in_specs=[pl.BlockSpec(memory_space=pltpu.HBM)] * 6,
        out_specs=[vmem, vmem],
        scratch_shapes=[
            pltpu.VMEM((8, 2, B, B), F32),
            pltpu.VMEM((8, 2, 4, B, B), F32),
            pltpu.VMEM((8, 4 * B, B), BF16),
            pltpu.VMEM((16 * B, 4 * B), BF16),
            pltpu.VMEM((4 * B, 16 * B), BF16),
            pltpu.VMEM((8, ROWS, B), F32),
            pltpu.VMEM((8, ROWS, B), F32),
            pltpu.VMEM((7, ROWS, B), F32),
            pltpu.VMEM((7, ROWS, B), F32),
            pltpu.SemaphoreType.DMA,
            pltpu.SemaphoreType.DMA((5,)),
            pltpu.SemaphoreType.DMA((LOTS,)),
        ],
        compiler_params=pltpu.CompilerParams(
            collective_id=0, has_side_effects=True, vmem_limit_bytes=32 << 20
        ),
    )(*(pltpu.with_memory_space_constraint(a, pltpu.HBM) for a in args))
    return pl.pallas_call(
        finish,
        out_shape=[shape, shape],
        in_specs=[vmem, vmem],
        out_specs=[vmem, vmem],
        compiler_params=pltpu.CompilerParams(vmem_limit_bytes=4 << 20),
    )(*sums)


def solution(mesh):
    rows, columns = P(None, ("pb", "ka"), None), P(None, ("ka", "pb"), None)
    return jax.shard_map(
        body,
        mesh=mesh,
        in_specs=(rows, columns, columns, rows, columns, columns),
        out_specs=(rows, rows),
        check_vma=False,
    )
```

```python
import math

import jax
import jax.numpy as jnp
from jax import lax
from jax.experimental import pallas as pl
from jax.experimental.pallas import tpu as pltpu
from jax.sharding import PartitionSpec as P

F32, BF16 = jnp.float32, jnp.bfloat16
MESH = pl.DeviceIdType.MESH
B = 128
H = 64
ROWS, DATA = 136, 8
PIECES = ((0, 72), (72, 64))
LOG2E = math.log2(math.e)
LOTS = 50


def split(x):
    high = x.astype(BF16)
    return high, (x - high.astype(F32)).astype(BF16)


def dot(a, b):
    return jnp.dot(a, b, preferred_element_type=F32)


def kernel(
    q_ref, k_ref, v_ref, dq_ref, dk_ref, dv_ref, num_out, tan_out,
    q_in, k_in, qt, kb, vt, num, tan, num_in, tan_in, own_sem, send_sem, recv_sem,
):
    pb, ka = lax.axis_index("pb"), lax.axis_index("ka")
    z, core = pb // 2, pb % 2
    x, y = ka // 4, ka % 4
    x_up = {"ka": ((x + 1) % 4) * 4 + y, "pb": pb}
    x_down = {"ka": ((x + 3) % 4) * 4 + y, "pb": pb}
    z_up = {"ka": ka, "pb": ((z + 1) % 4) * 2 + core}
    z_down = {"ka": ka, "pb": ((z + 3) % 4) * 2 + core}
    q_pair = {"ka": x * 4 + y + 1 - 2 * (y % 2), "pb": pb}
    k_pair = {"ka": x * 4 + 3 - y, "pb": pb}
    twin = {"ka": ka, "pb": z * 2 + 1 - core}

    for src, dst in (
        (q_ref, q_in.at[0, 0]), (dq_ref, q_in.at[0, 1]), (k_ref, k_in.at[0, 0, 0]),
        (dk_ref, k_in.at[0, 0, 1]), (v_ref, k_in.at[0, 0, 2]), (dv_ref, k_in.at[0, 0, 3]),
    ):
        pltpu.make_async_copy(src.at[0], dst, own_sem).start()
    barrier = pltpu.get_barrier_semaphore()
    peers = (x_up, x_down, z_up, z_down, q_pair, k_pair, twin)
    for peer in peers:
        pl.semaphore_signal(barrier, inc=1, device_id=peer, device_id_type=MESH)

    lots = {}

    def message(lot, group, src, dst, peer):
        n = lots.setdefault(lot, len(lots))
        return pltpu.make_async_remote_copy(
            src_ref=src, dst_ref=dst, send_sem=send_sem.at[group], recv_sem=recv_sem.at[n],
            device_id=peer, device_id_type=MESH,
        )

    def arrive(lot, size):
        pltpu.make_async_remote_copy(
            src_ref=size, dst_ref=size, send_sem=send_sem.at[0], recv_sem=recv_sem.at[lots[lot]],
            device_id=twin, device_id_type=MESH,
        ).wait_recv()

    def arrays(lot, count, rows=B):
        arrive(lot, k_in.at[:count, 0, 0, :rows])

    def begin(*copies):
        for copy in copies:
            copy.start()

    def q_message(a, src, dst, peer, lot=None):
        return message(lot or ("q", dst, a), 0, q_in.at[src, a], q_in.at[dst, a], peer)

    q1, q2, q3 = ((0, 0, 1, x_up), (0, 0, 2, x_down), (0, 0, 3, q_pair))
    qm = {
        (1, 0): q_message(*q1), (1, 1): q_message(1, 0, 1, x_up),
        (2, 0): q_message(*q2, "q near"), (2, 1): q_message(1, 0, 2, x_down),
        (3, 0): q_message(*q3), (3, 1): q_message(1, 0, 3, q_pair, "q near"),
        (4, 0): q_message(0, 3, 4, x_up, "q far"), (5, 0): q_message(0, 3, 5, x_down),
        (6, 0): q_message(0, 1, 6, x_up, "q far"), (7, 0): q_message(0, 5, 7, x_down, "q 7"),
        (4, 1): q_message(1, 1, 4, q_pair, "q far"), (5, 1): q_message(1, 2, 5, q_pair, "q far"),
        (6, 1): q_message(1, 1, 6, x_up), (7, 1): q_message(1, 6, 7, q_pair, "q 7"),
    }

    def half(s, c, a, h):
        return k_in.at[s, c, a, pl.ds(h * H, H)]

    near_lots = {
        (1, 2): "v1", (1, 3): "dv1", (2, 2): "v2", (2, 3): "v2",
        (1, 0): "k12", (1, 1): "k12", (2, 0): "k12", (2, 1): "k12",
    }
    near = {
        (s, a, h): message(near_lots[s, a] if h else "k near", 1, half(0, 0, a, h), half(s, 0, a, h), peer)
        for s, peer in ((1, z_up), (2, z_down))
        for a in range(4)
        for h in range(2)
    }

    def k_message(a, src, dst, peer, lot):
        return message(lot, 1, k_in.at[src, 0, a], k_in.at[dst, 0, a], peer)

    km = {}
    for a in range(2):
        km[3, a] = k_message(a, 0, 3, k_pair, ("k3", a))
        km[3, 2 + a] = k_message(2 + a, 0, 3, k_pair, "v3")
        km[4, a] = k_message(a, 3, 4, z_up, "k4")
        km[5, a] = k_message(a, 3, 5, z_down, ("k5", a))
        km[6, a] = k_message(a, 1, 6, z_up, "k6")
        km[7, a] = k_message(a, 5, 7, z_down, "k7")
        v = 2 + a
        km[4, v] = k_message(v, 1, 4, k_pair, "k4")
        km[5, v] = k_message(v, 2, 5, k_pair, "v5")
        km[6, v] = k_message(v, 1 + a, 6, (z_up, z_down)[a], ("v6", a))
        km[7, v] = k_message(v, 6, 7, k_pair, "v7")
    tm = {0: message("t0", 2, k_in.at[0, 0], k_in.at[0, 1], twin)}
    for s in (1, 2):
        for h in range(2):
            rows = pl.ds(h * H, H)
            tm[s, h] = message(("t near", h), 2, k_in.at[s, 0, :, rows], k_in.at[s, 1, :, rows], twin)
    for s in (3, 4, 5, 6, 7):
        for h in range(2):
            pair = pl.ds(2 * h, 2)
            lot = {3: ("t near", 1), 4: "t4", 5: "t56", 6: "t56", 7: "t7"}[s]
            tm[s, h] = message(lot, 2, k_in.at[s, 0, pair], k_in.at[s, 1, pair], twin)

    def whole(lot, group, src, dst, peer):
        return [message(lot, group, src, dst, peer)]

    def pieces(lot, group, src, dst, peer):
        return [
            message((lot, at), group, src.at[pl.ds(at, size)], dst.at[pl.ds(at, size)], peer)
            for at, size in PIECES
        ]

    nm = {
        "2": whole("n2", 3, num.at[6], num_in.at[0], x_up),
        "4": pieces("n4", 3, num.at[7], num_in.at[1], x_down),
        "3a": whole("n3", 3, num.at[5], num_in.at[2], x_up),
        "3b": pieces("n3b", 3, num.at[4], num_in.at[3], x_down),
        "0a": whole("n0", 3, num.at[2], num_in.at[4], x_up),
        "0b": whole("n0", 3, num.at[1], num_in.at[5], x_down),
        "0c": pieces("n0c", 3, num.at[3], num_in.at[6], q_pair),
    }
    dm = {
        "6": pieces("d6", 4, tan.at[7], tan_in.at[0], q_pair),
        "1": whole("d1", 4, tan.at[4], tan_in.at[1], q_pair),
        "2": whole("d2", 4, tan.at[5], tan_in.at[2], q_pair),
        "0": whole("d0", 4, tan.at[3], tan_in.at[3], q_pair),
        "2a": pieces("d2a", 4, tan.at[6], tan_in.at[4], x_up),
        "0a": pieces("d0a", 4, tan.at[2], tan_in.at[5], x_up),
        "0b": whole("d0", 4, tan.at[1], tan_in.at[6], x_down),
    }
    assert len(lots) == LOTS, len(lots)

    num[...] = jnp.zeros_like(num)
    tan[...] = jnp.zeros_like(tan)
    for s in range(8):
        num[s, :1] = jnp.full((1, B), -1e30, F32)
    own = k_in.at[:6, 0, 0]
    pltpu.make_async_copy(own, own, own_sem).wait()
    pl.semaphore_wait(barrier, len(peers))

    begin(qm[1, 1], qm[2, 1], qm[3, 0])
    for a in range(4):
        begin(km[3, a], near[1, a, 0], near[2, a, 0])
        if a == 0:
            begin(qm[1, 0], qm[2, 0], qm[3, 1], tm[0])
    for a in (2, 3, 0, 1):
        begin(near[1, a, 1], near[2, a, 1])

    scale = B**-0.5 * LOG2E

    def take_q(s):
        for a in range(2):
            high, low = split((q_in[s, a] * scale).T)
            qt[s, 2 * B * a : 2 * B * a + B] = high
            qt[s, 2 * B * a + B : 2 * B * a + 2 * B] = low

    def take_k(at, *parts):
        r = pl.ds(at * B, B)

        def read(a):
            got = [k_in[p[0], p[1], a] if len(p) == 2 else half(*p[:2], a, p[2])[...] for p in parts]
            return got[0] if len(got) == 1 else jnp.concatenate(got, axis=0)

        for a in range(2):
            high, low = split(read(a))
            kb[r, 2 * B * a : 2 * B * a + B] = high
            kb[r, 2 * B * a + B : 2 * B * a + 2 * B] = low
        for a in range(2):
            value = read(2 + a).T
            high, low = split(value * LOG2E if a else value)
            vt[2 * B * a : 2 * B * a + B, r] = high
            vt[2 * B * a + B : 2 * B * a + 2 * B, r] = low

    def step(first, blocks, side):
        r = pl.ds(pl.multiple_of(first * B, B), blocks * B)
        kk, dd = kb[r, : 2 * B], kb[r, 2 * B :]
        khigh = kk[:, :B]
        kd = jnp.concatenate([khigh, dd[:, :B]], axis=1)
        at = [side * 4 + j for j in range(4)]

        def wide(read):
            return jnp.concatenate([read(n) for n in at], axis=1)

        def sums(ref):
            return wide(lambda n: ref[n, DATA:])

        def stat(ref, row):
            return wide(lambda n: ref[n, row : row + 1])

        def put_sums(ref, value):
            for j, n in enumerate(at):
                ref[n, DATA:] = value[:, j * B : (j + 1) * B]

        def put_stat(ref, row, value):
            for j, n in enumerate(at):
                ref[n, row : row + 1] = value[:, j * B : (j + 1) * B]

        qhigh, qlow, dqhigh, dqlow = (
            wide(lambda n: qt[n, m * B : (m + 1) * B]) for m in range(4)
        )
        qq = jnp.concatenate([qhigh, qhigh], axis=0)
        s_ = dot(kk, qq) + dot(kk, jnp.concatenate([qlow, qlow], axis=0))
        t_ = (
            dot(kk, jnp.concatenate([dqhigh, dqhigh], axis=0))
            + dot(dd, qq)
            + dot(kd, jnp.concatenate([dqlow, qlow], axis=0))
        )
        old = stat(num, 0)
        new = jnp.maximum(old, jnp.max(s_, axis=0, keepdims=True))
        shrink = jnp.exp2(old - new)
        w = jnp.exp2(s_ - new)
        p = w * t_
        put_stat(num, 1, stat(num, 1) * shrink + jnp.sum(w, axis=0, keepdims=True))
        put_stat(tan, 1, stat(tan, 1) * shrink + jnp.sum(p, axis=0, keepdims=True))
        put_stat(num, 0, new)
        put_stat(tan, 0, new)
        whigh, wlow = split(w)
        phigh, plow = split(p)
        vhigh, vlow, dvhigh, dvlow = (vt[n * B : (n + 1) * B, r] for n in range(4))
        n_ = dot(vhigh, whigh) + dot(vlow, whigh) + dot(vhigh, wlow)
        d_ = (
            dot(dvhigh, whigh) + dot(dvlow, whigh) + dot(dvhigh, wlow)
            + dot(vhigh, phigh) + dot(vlow, phigh) + dot(vhigh, plow)
        )
        put_sums(num, sums(num) * shrink + n_)
        put_sums(tan, sums(tan) * shrink + d_)

    def early_0():
        take_q(0)
        take_k(0, (0, 0))
        arrays("t0", 4)
        take_k(1, (0, 1))
        arrays(("q", 1, 1), 1)
        begin(qm[6, 1], qm[4, 1])
        arrays(("q", 2, 1), 1)
        begin(qm[5, 1])
        arrays(("q", 3, 0), 1)
        begin(qm[4, 0], qm[5, 0])
        arrays(("q", 1, 0), 1)
        begin(qm[6, 0])
        arrays("q near", 2)
        arrays(("k3", 0), 1)
        begin(km[4, 0], km[5, 0])
        for s in (1, 2, 3):
            take_q(s)

    def early_1():
        arrays("k near", 4)
        begin(tm[1, 0], tm[2, 0])
        arrays(("k3", 1), 1)
        arrays("v1", 1, H)
        begin(km[6, 2], km[4, 2], km[4, 1], km[5, 1], tm[3, 0])
        take_k(2, (1, 0, 0), (2, 0, 0))
        arrays("dv1", 1, H)
        begin(km[4, 3])
        arrays("v2", 2, H)
        begin(km[6, 3], km[5, 2], km[5, 3])
        arrays(("q", 5, 0), 1)
        begin(qm[7, 0])
        arrays(("q", 6, 1), 1)
        begin(qm[7, 1])
        arrays(("t near", 0), 4)
        take_k(3, (1, 1, 0), (2, 1, 0))

    def early_2():
        arrays("k12", 4, H)
        begin(km[6, 0], km[6, 1], tm[1, 1], tm[2, 1])
        take_k(4, (1, 0, 1), (2, 0, 1))
        arrays("v3", 2)
        begin(tm[3, 1])
        take_k(5, (3, 0))

    def early_3():
        arrays(("t near", 1), 8)
        take_k(6, (1, 1, 1), (2, 1, 1))
        take_k(7, (3, 1))
        arrays(("k5", 0), 1)
        begin(km[7, 0])

    def late_0():
        arrays(("v6", 0), 1)
        begin(km[7, 2])
        arrays("q far", 4)
        for s in (4, 5, 6):
            take_q(s)
        arrays(("k5", 1), 1)
        begin(km[7, 1], tm[5, 0])
        arrays("q 7", 2)
        take_q(7)
        arrays(("v6", 1), 1)
        begin(km[7, 3], tm[6, 1])

    def late_1():
        arrays("k4", 4)
        begin(tm[4, 0], tm[4, 1])

    def late_2():
        arrays("v5", 2)
        begin(tm[5, 1])
        arrays("k6", 2)
        begin(tm[6, 0])
        arrays("t4", 4)
        for n, block in enumerate(((4, 0), (4, 1), (5, 0), (6, 0))):
            take_k(8 + n, block)

    def last_0():
        arrays("k7", 2)
        begin(tm[7, 0])
        arrays("v7", 2)
        begin(tm[7, 1])
        arrays("t56", 8)
        take_k(12, (5, 1))
        take_k(13, (6, 1))

    def last_1():
        arrays("t7", 4)
        take_k(14, (7, 0))
        take_k(15, (7, 1))

    def steps(events, first, blocks, side):
        def one(i, carry):
            for n, event in enumerate(events):
                pl.when(i == n)(event)
            step(first + blocks * i, blocks, side)
            return carry

        return one

    lax.fori_loop(0, 4, steps((early_0, early_1, early_2, early_3), 0, 2, 0), 0)
    lax.fori_loop(0, 3, steps((late_0, late_1, late_2), 0, 4, 1), 0)
    lax.fori_loop(0, 2, steps((last_0, last_1), 12, 2, 1), 0)
    begin(*nm["4"], *dm["6"], *nm["2"], *dm["1"], *nm["3a"], *dm["2"])
    lax.fori_loop(0, 2, steps((), 8, 4, 0), 0)

    def join(ref, s, other):
        old, got = ref[s, :1], other[:1]
        peak = jnp.maximum(old, got)
        mine, theirs = jnp.exp2(old - peak), jnp.exp2(got - peak)
        for n, (at, size) in enumerate(PIECES):
            r = pl.ds(at, size)
            ref[s, r] = ref[s, r] * mine + other[r] * theirs
            if n == 0:
                ref[s, :1] = peak
            yield

    def add(copies, ref, s, other, then=()):
        for copy in copies:
            copy.wait_recv()
        for _ in join(ref, s, other):
            pass
        begin(*then)

    def relay(*chains):
        joins = [join(ref, s, other) for _, ref, s, other, _ in chains]
        for n in range(len(PIECES)):
            for part, (copies, _, _, _, then) in zip(joins, chains):
                copies[n].wait_recv()
                next(part, None)
                begin(*then[n : n + 1])

    begin(*dm["0"])
    relay((dm["6"], tan, 6, tan_in.at[0], dm["2a"]), (nm["4"], num, 4, num_in.at[1], nm["3b"]))
    begin(*nm["0b"])
    add(nm["2"], num, 2, num_in.at[0], nm["0a"])
    add(dm["1"], tan, 1, tan_in.at[1], dm["0b"])
    add(nm["3a"], num, 3, num_in.at[2])
    add(dm["2"], tan, 2, tan_in.at[2])
    relay((dm["2a"], tan, 2, tan_in.at[4], dm["0a"]), (nm["3b"], num, 3, num_in.at[3], nm["0c"]))
    arrive("n0", num_in.at[:2])
    add((), num, 0, num_in.at[5])
    add((), num, 0, num_in.at[4])
    relay((dm["0a"], tan, 0, tan_in.at[5], ()), (nm["0c"], num, 0, num_in.at[6], ()))
    arrive("d0", tan_in.at[:2])
    add((), tan, 0, tan_in.at[3])
    add((), tan, 0, tan_in.at[6])
    num_out[...] = num[0]
    tan_out[...] = tan[0]
    for group, size in enumerate((q_in.at[:7], k_in.at[:7, 0], k_in.at[:, 1], num_in, tan_in)):
        pltpu.make_async_remote_copy(
            src_ref=size, dst_ref=size, send_sem=send_sem.at[group], recv_sem=recv_sem.at[0],
            device_id=twin, device_id_type=MESH,
        ).wait_send()


def finish(num, tan, out_ref, tout_ref):
    inverse = 1.0 / num[1:2]
    attended = num[DATA:] * inverse
    moved = (tan[DATA:] * inverse - attended * (tan[1:2] * inverse)) * (1.0 / LOG2E)
    out_ref[0] = attended.T
    tout_ref[0] = moved.T


def body(*args):
    sums = jax.ShapeDtypeStruct((ROWS, B), F32)
    shape = jax.ShapeDtypeStruct((1, B, B), F32)
    vmem = pl.BlockSpec(memory_space=pltpu.VMEM)
    sums = pl.pallas_call(
        kernel,
        out_shape=[sums, sums],
        in_specs=[pl.BlockSpec(memory_space=pltpu.HBM)] * 6,
        out_specs=[vmem, vmem],
        scratch_shapes=[
            pltpu.VMEM((8, 2, B, B), F32),
            pltpu.VMEM((8, 2, 4, B, B), F32),
            pltpu.VMEM((8, 4 * B, B), BF16),
            pltpu.VMEM((16 * B, 4 * B), BF16),
            pltpu.VMEM((4 * B, 16 * B), BF16),
            pltpu.VMEM((8, ROWS, B), F32),
            pltpu.VMEM((8, ROWS, B), F32),
            pltpu.VMEM((7, ROWS, B), F32),
            pltpu.VMEM((7, ROWS, B), F32),
            pltpu.SemaphoreType.DMA,
            pltpu.SemaphoreType.DMA((5,)),
            pltpu.SemaphoreType.DMA((LOTS,)),
        ],
        compiler_params=pltpu.CompilerParams(
            collective_id=0, has_side_effects=True, vmem_limit_bytes=32 << 20
        ),
    )(*(pltpu.with_memory_space_constraint(a, pltpu.HBM) for a in args))
    return pl.pallas_call(
        finish,
        out_shape=[shape, shape],
        in_specs=[vmem, vmem],
        out_specs=[vmem, vmem],
        compiler_params=pltpu.CompilerParams(vmem_limit_bytes=4 << 20),
    )(*sums)


def solution(mesh):
    rows, columns = P(None, ("pb", "ka"), None), P(None, ("ka", "pb"), None)
    return jax.shard_map(
        body,
        mesh=mesh,
        in_specs=(rows, columns, columns, rows, columns, columns),
        out_specs=(rows, rows),
        check_vma=False,
    )
```
